16 devices in a mesh: dp: 2 (over y, z), tp: 8 (over x, core).
Axes of the slice: x: 4, y: 2, z: 1, core: 2. Of those that a mesh axis runs over, the one named last changes fastest.
The devices are a block of a 4x4x8 slice.
Arguments:
- hidden: bfloat16 [256, 5120], P('dp'), parts along dimension 0
- lengths: int32 [256], P('dp'), parts along dimension 0
- k_cache: bfloat16 [2, 256, 128, 8, 128], P(None, 'dp', None, 'tp'), parts along dimension 1
- v_cache: bfloat16 [2, 256, 128, 8, 128], P(None, 'dp', None, 'tp'), parts along dimension 1
- attn_norm: bfloat16 [2, 5120], replicated
- w_qkv: bfloat16 [2, 5120, 8, 768], P(None, None, 'tp')
- w_out: bfloat16 [2, 4096, 5120], P(None, 'tp')
- mlp_norm: bfloat16 [2, 5120], replicated
- w_gate: bfloat16 [2, 5120, 14336], P(None, None, 'tp')
- w_up: bfloat16 [2, 5120, 14336], P(None, None, 'tp')
- w_down: bfloat16 [2, 14336, 5120], P(None, 'tp')
Outputs:
- output: bfloat16 [256, 5120], P('dp'), parts along dimension 0
There are 2 independent parts. The reference program is written for one: setup_inputs(seed, part) draws one part's arguments, and reference() takes and returns one part's arrays. A program takes and returns all parts, laid end to end along the dimension named above; an argument that names none is the same for every part.
All inputs are finite; a program needn't handle non-finite values.
Results may differ from the reference program's by a relative error of at most 0.0187289.
Values are sent between devices in bfloat16 or wider.
A program may use at most 768 MiB of HBM per device.

```python
import jax
import jax.numpy as jnp
from jax import lax

D_MODEL = 5120
HEADS = 32
KV_HEADS = 8
HEAD_DIM = 128
FF_DIM = 14336
BATCH = 128
SEQ_LEN = 128
LAYERS = 2
GROUP_DEVS = 8
GROUP = HEADS // KV_HEADS
ROPE_BASE = 10000.0
NORM_EPS = 1e-5


def setup_inputs(seed: int = 0, part: int = 0) -> dict:
    base_key = jax.random.key(seed)
    part_key = jax.random.fold_in(base_key, part)
    keys = jax.random.split(part_key, 8)
    weight_keys = jax.random.split(base_key, 8)
    row_ids = jnp.arange(BATCH)
    long_count = max(1, BATCH // 8)
    long_len = jax.random.randint(keys[0], (BATCH,), SEQ_LEN // 2, SEQ_LEN)
    short_len = jax.random.randint(keys[1], (BATCH,), 1, SEQ_LEN // 16 + 1)
    lengths = jnp.where(row_ids < long_count, long_len, short_len)
    lengths = jnp.where(row_ids == 0, SEQ_LEN - 1, jnp.where(row_ids == BATCH - 1, 1, lengths)).astype(jnp.int32)
    hidden = jax.random.normal(keys[2], (BATCH, D_MODEL), jnp.float32).astype(jnp.bfloat16)
    cache_shape = (LAYERS, BATCH, SEQ_LEN, KV_HEADS, HEAD_DIM)
    mean_shape = (LAYERS, BATCH, 1, KV_HEADS, HEAD_DIM)
    k_cache = (1.5 * jax.random.normal(keys[3], cache_shape, jnp.float32)).astype(jnp.bfloat16)
    mean_live = jax.random.normal(keys[4], mean_shape, jnp.float32)
    mean_stale = jax.random.normal(keys[5], mean_shape, jnp.float32)
    live = jnp.arange(SEQ_LEN)[None, None, :, None, None] < lengths[None, :, None, None, None]
    noise = jax.random.normal(keys[6], cache_shape, jnp.float32)
    v_cache = (0.6 * jnp.where(live, mean_live, mean_stale) + 0.8 * noise).astype(jnp.bfloat16)
    qo_dim = HEADS * HEAD_DIM
    attn_norm = jax.random.uniform(weight_keys[0], (LAYERS, D_MODEL), jnp.float32, 0.5, 1.5).astype(jnp.bfloat16)
    w_qkv = (jax.random.normal(weight_keys[1], (LAYERS, D_MODEL, KV_HEADS, (GROUP + 2) * HEAD_DIM), jnp.float32) * D_MODEL ** -0.5).astype(jnp.bfloat16)
    w_out = (jax.random.normal(weight_keys[2], (LAYERS, qo_dim, D_MODEL), jnp.float32) * qo_dim ** -0.5).astype(jnp.bfloat16)
    mlp_norm = jax.random.uniform(weight_keys[3], (LAYERS, D_MODEL), jnp.float32, 0.5, 1.5).astype(jnp.bfloat16)
    w_gate = (jax.random.normal(weight_keys[4], (LAYERS, D_MODEL, FF_DIM), jnp.float32) * D_MODEL ** -0.5).astype(jnp.bfloat16)
    w_up = (jax.random.normal(weight_keys[5], (LAYERS, D_MODEL, FF_DIM), jnp.float32) * D_MODEL ** -0.5).astype(jnp.bfloat16)
    w_down = (jax.random.normal(weight_keys[6], (LAYERS, FF_DIM, D_MODEL), jnp.float32) * FF_DIM ** -0.5).astype(jnp.bfloat16)
    return {'hidden': hidden, 'lengths': lengths, 'k_cache': k_cache, 'v_cache': v_cache,
            'attn_norm': attn_norm, 'w_qkv': w_qkv, 'w_out': w_out, 'mlp_norm': mlp_norm,
            'w_gate': w_gate, 'w_up': w_up, 'w_down': w_down}


def rms_norm(values, gain):
    wide = values.astype(jnp.float32)
    scale = lax.rsqrt(jnp.mean(wide * wide, axis=-1, keepdims=True) + NORM_EPS)
    return (wide * scale * gain.astype(jnp.float32)).astype(jnp.bfloat16)


def rotate(values, cosine, sine):
    half = values.shape[-1] // 2
    first = values[..., :half]
    second = values[..., half:]
    return jnp.concatenate([first * cosine - second * sine, second * cosine + first * sine], axis=-1)


def attend_row(row_data):
    query, key_new, val_new, keys_row, values_row, length = row_data
    scale = HEAD_DIM ** -0.5
    query_wide = query.astype(jnp.float32)
    logits = jnp.einsum('kgd,skd->kgs', query_wide, keys_row.astype(jnp.float32)) * scale
    live = jnp.arange(SEQ_LEN) < length
    logits = jnp.where(live[None, None, :], logits, -1e30)
    self_logit = jnp.einsum('kgd,kd->kg', query_wide, key_new.astype(jnp.float32)) * scale
    peak = jnp.maximum(jnp.max(logits, axis=-1), self_logit)
    weights = jnp.exp(logits - peak[..., None]).astype(jnp.bfloat16).astype(jnp.float32)
    self_weight = jnp.exp(self_logit - peak).astype(jnp.bfloat16).astype(jnp.float32)
    denominator = jnp.sum(weights, axis=-1) + self_weight
    numerator = jnp.einsum('kgs,skd->kgd', weights, values_row.astype(jnp.float32))
    numerator = numerator + self_weight[..., None] * val_new.astype(jnp.float32)[:, None, :]
    return (numerator / denominator[..., None]).astype(jnp.bfloat16)


def reference(hidden, lengths, k_cache, v_cache, attn_norm, w_qkv, w_out, mlp_norm, w_gate, w_up, w_down):
    inv_freq = ROPE_BASE ** (-jnp.arange(0, HEAD_DIM, 2, dtype=jnp.float32) / HEAD_DIM)
    angles = lengths.astype(jnp.float32)[:, None] * inv_freq[None, :]
    cosine = jnp.cos(angles)
    sine = jnp.sin(angles)

    def layer_step(residual, layer_data):
        cache_k, cache_v, gain_attn, qkv_layer, out_layer, gain_mlp, gate_layer, up_layer, down_layer = layer_data
        normed = rms_norm(residual, gain_attn)
        fused = jnp.dot(normed, qkv_layer.reshape(D_MODEL, -1), preferred_element_type=jnp.float32).astype(jnp.bfloat16)
        fused = fused.reshape(BATCH, KV_HEADS, GROUP + 2, HEAD_DIM).astype(jnp.float32)
        query = rotate(fused[:, :, :GROUP], cosine[:, None, None, :], sine[:, None, None, :]).astype(jnp.bfloat16)
        key_new = rotate(fused[:, :, GROUP], cosine[:, None, :], sine[:, None, :]).astype(jnp.bfloat16)
        val_new = fused[:, :, GROUP + 1].astype(jnp.bfloat16)
        attended = lax.map(attend_row, (query, key_new, val_new, cache_k, cache_v, lengths))
        attended = attended.reshape(BATCH, GROUP_DEVS, -1).astype(jnp.float32)
        out_parts = jnp.einsum('btf,tfd->btd', attended, out_layer.reshape(GROUP_DEVS, -1, D_MODEL).astype(jnp.float32)).astype(jnp.bfloat16)
        after_attn = (residual.astype(jnp.float32) + jnp.sum(out_parts.astype(jnp.float32), axis=1)).astype(jnp.bfloat16)
        normed_mlp = rms_norm(after_attn, gain_mlp)
        gate_proj = jnp.dot(normed_mlp, gate_layer, preferred_element_type=jnp.float32).astype(jnp.bfloat16)
        up_proj = jnp.dot(normed_mlp, up_layer, preferred_element_type=jnp.float32).astype(jnp.bfloat16)
        activated = (jax.nn.silu(gate_proj.astype(jnp.float32)) * up_proj.astype(jnp.float32)).astype(jnp.bfloat16)
        activated = activated.reshape(BATCH, GROUP_DEVS, -1).astype(jnp.float32)
        down_parts = jnp.einsum('btf,tfd->btd', activated, down_layer.reshape(GROUP_DEVS, -1, D_MODEL).astype(jnp.float32)).astype(jnp.bfloat16)
        layer_out = (after_attn.astype(jnp.float32) + jnp.sum(down_parts.astype(jnp.float32), axis=1)).astype(jnp.bfloat16)
        return layer_out, None

    final, _ = lax.scan(layer_step, hidden, (k_cache, v_cache, attn_norm, w_qkv, w_out, mlp_norm, w_gate, w_up, w_down))
    return final
```

```python
import functools

import jax
import jax.numpy as jnp
from jax import lax
from jax.experimental import pallas as pl
from jax.experimental.pallas import tpu as pltpu
from jax.sharding import PartitionSpec as P

ROPE_BASE = 10000.0
NORM_EPS = 1e-5
F32 = jnp.float32
BF16 = jnp.bfloat16
MESH = pl.DeviceIdType.MESH
CORES = 2
GU_SLOTS = 5
DN_SLOTS = 2
NEG = -1e30


def rope_tables(lengths, head_dim):
    inv_freq = ROPE_BASE ** (-jnp.arange(0, head_dim, 2, dtype=F32) / head_dim)
    angles = lengths.astype(F32)[:, None] * inv_freq[None, :]
    cosine, sine = jnp.cos(angles), jnp.sin(angles)
    return jnp.concatenate([cosine, cosine], 1), jnp.concatenate([-sine, sine], 1)


def kernel(cfg, hid, lens, cos_ref, sin_ref, gain_attn, gain_mlp, wqkv, wout, wgate, wup, wdown, kc, vc, out,
           x, a_buf, rbuf, lrep, part, rel_in, prt_in, dir_in, own_in, f_out, f_in, stat,
           q_s, kn_s, vn_s, s_s, attn, act, g_acc, u_acc,
           b_qkv, b_out, b_k, b_v, b_gu, b_d,
           rs_sem, ag_sem, st_sem, snd_sem, snd2_sem, w_sem, x_sem):
    layers, rows, width, head_dim, group, chips, seq = cfg
    half = rows // 2
    wide = CORES * width
    qkv_cols = (group + 2) * head_dim
    d_model = chips * wide
    tp = lax.axis_index('tp')
    e = lax.rem(tp, CORES)
    c = lax.div(tp, CORES)
    other = 1 - e
    right = lax.rem(c + 1, chips)
    left = lax.rem(c + chips - 1, chips)
    far = lax.rem(c + 2, chips)
    first = pl.ds(0, half)
    second = pl.ds(half, half)

    def dev(chip, core):
        return {'tp': chip * CORES + core}

    def cols(chip):
        return pl.ds(pl.multiple_of(chip * wide, wide), wide)

    in_order = (c, left, right, far)
    out_order = (far, right, left, c)

    def ld_qkv(l, i):
        return pltpu.make_async_copy(wqkv.at[l, cols(in_order[i]), :], b_qkv.at[i], w_sem.at[i])

    def ld_out(l, i):
        return pltpu.make_async_copy(wout.at[l, :, cols(out_order[i])], b_out.at[i], w_sem.at[4 + i])

    def ld_k(l):
        return pltpu.make_async_copy(kc.at[l], b_k, w_sem.at[8])

    def ld_v(l):
        return pltpu.make_async_copy(vc.at[l], b_v, w_sem.at[9])

    def ld_gu(m):
        l, i, s = m // (2 * chips), m // 2 % chips, m % GU_SLOTS
        src = wup if m % 2 else wgate
        return pltpu.make_async_copy(src.at[l, cols(in_order[i]), :], b_gu.at[s], w_sem.at[10 + s])

    def ld_d(n):
        l, i, s = n // chips, n % chips, n % DN_SLOTS
        return pltpu.make_async_copy(wdown.at[l, :, cols(out_order[i])], b_d.at[s], w_sem.at[10 + GU_SLOTS + s])

    x_loads = [pltpu.make_async_copy(
        hid.at[:, pl.ds(k * wide + h * width, width)], x.at[k, h], x_sem.at[k, h])
        for k in range(chips) for h in range(CORES)]
    for cp in x_loads:
        cp.start()
    for i in range(chips):
        ld_qkv(0, i).start()
    ld_k(0).start()
    ld_v(0).start()
    for i in range(chips):
        ld_out(0, i).start()

    barrier = pltpu.get_barrier_semaphore()
    n_dev = chips * CORES
    for step in range(1, n_dev):
        pl.semaphore_signal(barrier, inc=1, device_id={'tp': lax.rem(tp + step, n_dev)}, device_id_type=MESH)
    pl.semaphore_wait(barrier, n_dev - 1)

    lens_row = jnp.broadcast_to(lens[...].astype(F32), (rows, rows)).T
    for g in range(group):
        lrep[pl.ds(g, rows, stride=group), :] = lens_row

    for cp in x_loads:
        cp.wait()
    total = jnp.zeros((rows, 128), F32)
    for k in range(chips):
        for h in range(CORES):
            for j in range(width // 128):
                v = x[k, h, :, j * 128:(j + 1) * 128].astype(F32)
                total = total + v * v
    scale0 = lax.rsqrt(jnp.sum(total, axis=1, keepdims=True) / d_model + NORM_EPS)
    rbuf[...] = jnp.broadcast_to(scale0, (rows, 128))

    def normed(chip, gain_ref, l):
        r = jnp.concatenate([rbuf[...]] * (width // 128), axis=1)
        gain = gain_ref[l:l + 1, cols(chip)].astype(F32)
        for h in range(CORES):
            piece = x[chip, h].astype(F32)
            a_buf[:, h * width:(h + 1) * width] = (
                piece * r * gain[:, h * width:(h + 1) * width]).astype(BF16)

    def use_qkv(l):
        def consume(i):
            normed(in_order[i], gain_attn, l)
            ld_qkv(l, i).wait()
            prod = jnp.dot(a_buf[...], b_qkv[i], preferred_element_type=F32)
            if i == 0:
                g_acc[:, :qkv_cols] = prod
            else:
                g_acc[:, :qkv_cols] += prod
            if l + 1 < layers:
                ld_qkv(l + 1, i).start()
        return consume

    def use_gu(l):
        def consume(i):
            normed(in_order[i], gain_mlp, l)
            for j, acc in enumerate((g_acc, u_acc)):
                m = 2 * (l * chips + i) + j
                ld_gu(m).wait()
                prod = jnp.dot(a_buf[...], b_gu[m % GU_SLOTS], preferred_element_type=F32)
                if i == 0:
                    acc[...] = prod
                else:
                    acc[...] += prod
                if m + GU_SLOTS < layers * chips * 2:
                    ld_gu(m + GU_SLOTS).start()
        return consume

    def attention(l):
        cosine, sine = cos_ref[...], sin_ref[...]

        def rot(v):
            return (v * cosine + pltpu.roll(v, head_dim // 2, 1) * sine).astype(BF16).astype(F32)

        def head(j):
            return g_acc[:, j * head_dim:(j + 1) * head_dim].astype(BF16).astype(F32)

        key_new = rot(head(group))
        val_new = head(group + 1)
        for g in range(group):
            at = pl.ds(g, rows, stride=group)
            q_s[at, :] = rot(head(g))
            kn_s[at, :] = key_new
            vn_s[at, :] = val_new
        scale = head_dim ** -0.5
        pair = 2 * group
        upper = lax.broadcasted_iota(jnp.int32, (pair, head_dim), 0) < group
        ld_k(l).wait()

        def scores(i, carry):
            at = pl.ds(pl.multiple_of(i * pair, pair), pair)
            q = q_s[at, :].astype(BF16)
            keys = b_k[pl.ds(i * 2, 2)].reshape(2 * seq, head_dim)
            s = lax.dot_general(q, keys, (((1,), (1,)), ((), ())), preferred_element_type=F32)
            s_s[at, :] = jnp.where(upper, s[:, :seq], s[:, seq:])
            return carry

        lax.fori_loop(0, rows // 2, scores, 0, unroll=8)
        if l + 1 < layers:
            ld_k(l + 1).start()
        pos = lax.broadcasted_iota(jnp.int32, (rows * group, seq), 1).astype(F32)
        s = jnp.where(pos < lrep[...], s_s[...] * scale, NEG)
        own = jnp.sum(q_s[...] * kn_s[...], axis=1, keepdims=True) * scale
        peak = jnp.maximum(jnp.max(s, axis=1, keepdims=True), own)
        w = jnp.exp(s - peak).astype(BF16).astype(F32)
        w_own = jnp.exp(own - peak).astype(BF16).astype(F32)
        denom = jnp.sum(w, axis=1, keepdims=True) + w_own
        s_s[...] = w
        q_s[...] = w_own * vn_s[...]
        kn_s[...] = jnp.broadcast_to(denom, kn_s.shape)
        ld_v(l).wait()

        def mix(i, carry):
            at = pl.ds(pl.multiple_of(i * pair, pair), pair)
            w = s_s[at, :].astype(BF16)
            vals = jnp.concatenate([b_v[i * 2], b_v[i * 2 + 1]], axis=1)
            o = jnp.dot(w, vals, preferred_element_type=F32)
            o = jnp.where(upper, o[:, :head_dim], o[:, head_dim:])
            s_s[at, :] = (o + q_s[at, :]) / kn_s[at, :]
            return carry

        lax.fori_loop(0, rows // 2, mix, 0, unroll=8)
        if l + 1 < layers:
            ld_v(l + 1).start()
        for g in range(group):
            attn[:, g * head_dim:(g + 1) * head_dim] = s_s[pl.ds(g, rows, stride=group), :].astype(BF16)

    def chunk_out(l):
        def chunk(i):
            ld_out(l, i).wait()
            prod = jnp.dot(attn[...], b_out[i], preferred_element_type=F32)
            part[i, 0] = prod[:, :width].astype(BF16)
            part[i, 1] = prod[:, width:].astype(BF16)
            if l + 1 < layers:
                ld_out(l + 1, i).start()
        return chunk

    def chunk_down(l):
        def chunk(i):
            n = l * chips + i
            ld_d(n).wait()
            prod = jnp.dot(act[...], b_d[n % DN_SLOTS], preferred_element_type=F32)
            part[i, 0] = prod[:, :width].astype(BF16)
            part[i, 1] = prod[:, width:].astype(BF16)
            if n + DN_SLOTS < layers * chips:
                ld_d(n + DN_SLOTS).start()
        return chunk

    def reduce_scatter(chunk):
        sends = []

        def send(src, dst, rsem, where):
            cp = pltpu.make_async_remote_copy(
                src_ref=src, dst_ref=dst, send_sem=snd_sem.at[len(sends)], recv_sem=rsem,
                device_id=where, device_id_type=MESH)
            cp.start()
            sends.append(cp)

        def arrived(dst, rsem):
            pltpu.make_async_remote_copy(
                src_ref=dst, dst_ref=dst, send_sem=snd_sem.at[0], recv_sem=rsem,
                device_id=dev(c, e), device_id_type=MESH).wait_recv()

        chunk(0)
        for q in range(CORES):
            send(part.at[0, q, first], rel_in.at[0, e], rs_sem.at[e], dev(right, q))
            send(part.at[0, q, second], rel_in.at[1, e], rs_sem.at[2 + e], dev(left, q))
        chunk(1)
        send(part.at[1, other, first], prt_in.at[0], rs_sem.at[4], dev(c, other))
        for q in range(CORES):
            send(part.at[1, q, second], dir_in.at[1, e], rs_sem.at[8 + e], dev(right, q))
        chunk(2)
        send(part.at[2, other, second], prt_in.at[1], rs_sem.at[5], dev(c, other))
        for q in range(CORES):
            send(part.at[2, q, first], dir_in.at[0, e], rs_sem.at[6 + e], dev(left, q))
        chunk(3)
        send(part.at[3, other], own_in, rs_sem.at[12], dev(c, other))
        for way in range(2):
            where = (first, second)[way]
            for q in range(CORES):
                arrived(rel_in.at[way, q], rs_sem.at[2 * way + q])
            arrived(prt_in.at[way], rs_sem.at[4 + way])
            f_out[way] = (rel_in[way, 0].astype(F32) + rel_in[way, 1].astype(F32)
                          + (prt_in[way].astype(F32) + part[1 + way, e, where].astype(F32)))
            send(f_out.at[way], f_in.at[way], rs_sem.at[10 + way], dev((right, left)[way], e))
        arrived(own_in, rs_sem.at[12])
        squares = []
        for way in range(2):
            where = (first, second)[way]
            for q in range(CORES):
                arrived(dir_in.at[way, q], rs_sem.at[6 + 2 * way + q])
            arrived(f_in.at[way], rs_sem.at[10 + way])
            h = ((part[3, e, where].astype(F32) + own_in[where].astype(F32))
                 + (dir_in[way, 0].astype(F32) + dir_in[way, 1].astype(F32)) + f_in[way])
            h = (x[c, e, where].astype(F32) + h).astype(BF16)
            x[c, e, where] = h
            h = h.astype(F32)
            sq = h * h
            tot = sq[:, :128]
            for j in range(1, width // 128):
                tot = tot + sq[:, j * 128:(j + 1) * 128]
            squares.append(tot)
        for cp in sends:
            cp.wait_send()
        return jnp.concatenate(squares, axis=0)

    def all_gather(squares, consume):
        sends = []

        def send(src, dst, rsem, where):
            cp = pltpu.make_async_remote_copy(
                src_ref=src, dst_ref=dst, send_sem=snd2_sem.at[len(sends)], recv_sem=rsem,
                device_id=where, device_id_type=MESH)
            cp.start()
            sends.append(cp)

        def arrived(dst, rsem):
            pltpu.make_async_remote_copy(
                src_ref=dst, dst_ref=dst, send_sem=snd2_sem.at[0], recv_sem=rsem,
                device_id=dev(c, e), device_id_type=MESH).wait_recv()

        ranges = (first, second)

        def push(chip, core, way, where):
            ref = x.at[chip, core, ranges[way]]
            send(ref, ref, ag_sem.at[chip, core, way], where)

        def have(chip, core, way):
            arrived(x.at[chip, core, ranges[way]], ag_sem.at[chip, core, way])

        if squares is not None:
            row = jnp.sum(squares.T, axis=0, keepdims=True)
            stat[tp] = jnp.broadcast_to(row, (8, rows))
            for step in range(1, n_dev):
                send(stat.at[tp], stat.at[tp], st_sem.at[tp], {'tp': lax.rem(tp + step, n_dev)})
        push(c, e, 0, dev(right, e))
        push(c, e, 1, dev(left, e))
        push(c, e, 1, dev(right, e))
        push(c, e, 0, dev(left, e))
        push(c, e, 0, dev(c, other))
        push(c, e, 1, dev(c, other))
        if squares is not None:
            for step in range(1, n_dev):
                src = lax.rem(tp + step, n_dev)
                arrived(stat.at[src], st_sem.at[src])
            row = stat[0, 0:1]
            for j in range(1, n_dev):
                row = row + stat[j, 0:1]
            rbuf[...] = jnp.broadcast_to(lax.rsqrt(row / d_model + NORM_EPS), (rows, rows)).T
        have(c, other, 0)
        have(c, other, 1)
        consume(0)
        have(left, e, 0)
        push(left, e, 0, dev(right, e))
        push(left, e, 0, dev(c, other))
        have(right, e, 1)
        push(right, e, 1, dev(left, e))
        push(right, e, 1, dev(c, other))
        have(left, e, 1)
        push(left, e, 1, dev(c, other))
        have(right, e, 0)
        push(right, e, 0, dev(c, other))
        have(left, other, 0)
        have(left, other, 1)
        consume(1)
        have(far, e, 0)
        push(far, e, 0, dev(c, other))
        have(far, e, 1)
        push(far, e, 1, dev(c, other))
        have(right, other, 0)
        have(right, other, 1)
        consume(2)
        have(far, other, 0)
        have(far, other, 1)
        consume(3)
        for cp in sends:
            cp.wait_send()

    for i in range(chips):
        use_qkv(0)(i)
    for m in range(GU_SLOTS):
        ld_gu(m).start()
    for l in range(layers):
        attention(l)
        if l == 0:
            for n in range(DN_SLOTS):
                ld_d(n).start()
        squares = reduce_scatter(chunk_out(l))
        all_gather(squares, use_gu(l))
        gate = g_acc[...].astype(BF16).astype(F32)
        up = u_acc[...].astype(BF16).astype(F32)
        act[...] = (gate * jax.nn.sigmoid(gate) * up).astype(BF16)
        squares = reduce_scatter(chunk_down(l))
        if l + 1 < layers:
            all_gather(squares, use_qkv(l + 1))
    stores = []

    def store(i):
        for h in range(CORES):
            cp = pltpu.make_async_copy(
                x.at[in_order[i], h],
                out.at[:, pl.ds(pl.multiple_of(in_order[i] * wide + h * width, width), width)],
                x_sem.at[i, h])
            cp.start()
            stores.append(cp)

    all_gather(None, store)
    for cp in stores:
        cp.wait()


def solution(mesh):
    n_dev = mesh.shape['tp']
    chips = n_dev // CORES

    def local_step(hidden, lengths, k_cache, v_cache, attn_norm, w_qkv, w_out, mlp_norm, w_gate, w_up, w_down):
        layers, rows, seq, _, head_dim = k_cache.shape
        d_model = hidden.shape[1]
        width = d_model // n_dev
        qkv_cols = w_qkv.shape[3]
        group = qkv_cols // head_dim - 2
        ff = w_gate.shape[2]
        half = rows // 2
        wide = CORES * width
        heads = group * head_dim
        cosine, sine = rope_tables(lengths, head_dim)
        cfg = (layers, rows, width, head_dim, group, chips, seq)
        vmem = pl.BlockSpec(memory_space=pltpu.VMEM)
        hbm = pl.BlockSpec(memory_space=pl.ANY)
        flops = 2 * layers * rows * d_model * (qkv_cols + heads + 3 * ff)
        return pl.pallas_call(
            functools.partial(kernel, cfg),
            out_shape=jax.ShapeDtypeStruct((rows, d_model), BF16),
            in_specs=[hbm] + [vmem] * 5 + [hbm] * 7,
            out_specs=hbm,
            scratch_shapes=[
                pltpu.VMEM((chips, CORES, rows, width), BF16),
                pltpu.VMEM((rows, wide), BF16),
                pltpu.VMEM((rows, 128), F32),
                pltpu.VMEM((rows * group, seq), F32),
                pltpu.VMEM((chips, CORES, rows, width), BF16),
                pltpu.VMEM((2, CORES, half, width), BF16),
                pltpu.VMEM((2, half, width), BF16),
                pltpu.VMEM((2, CORES, half, width), BF16),
                pltpu.VMEM((rows, width), BF16),
                pltpu.VMEM((2, half, width), F32),
                pltpu.VMEM((2, half, width), F32),
                pltpu.VMEM((n_dev, 8, rows), F32),
                pltpu.VMEM((rows * group, head_dim), F32),
                pltpu.VMEM((rows * group, head_dim), F32),
                pltpu.VMEM((rows * group, head_dim), F32),
                pltpu.VMEM((rows * group, seq), F32),
                pltpu.VMEM((rows, heads), BF16),
                pltpu.VMEM((rows, ff), BF16),
                pltpu.VMEM((rows, ff), F32),
                pltpu.VMEM((rows, ff), F32),
                pltpu.VMEM((chips, wide, qkv_cols), BF16),
                pltpu.VMEM((chips, heads, wide), BF16),
                pltpu.VMEM((rows, seq, head_dim), BF16),
                pltpu.VMEM((rows, seq, head_dim), BF16),
                pltpu.VMEM((GU_SLOTS, wide, ff), BF16),
                pltpu.VMEM((DN_SLOTS, ff, wide), BF16),
                pltpu.SemaphoreType.DMA((13,)),
                pltpu.SemaphoreType.DMA((chips, CORES, 2)),
                pltpu.SemaphoreType.DMA((n_dev,)),
                pltpu.SemaphoreType.DMA((16,)),
                pltpu.SemaphoreType.DMA((24,)),
                pltpu.SemaphoreType.DMA((10 + GU_SLOTS + DN_SLOTS,)),
                pltpu.SemaphoreType.DMA((chips, CORES)),
            ],
            compiler_params=pltpu.CompilerParams(
                collective_id=0, has_side_effects=True, vmem_limit_bytes=67043328),
            cost_estimate=pl.CostEstimate(flops=flops, bytes_accessed=flops // rows, transcendentals=0),
        )(hidden, lengths.reshape(1, rows), cosine, sine, attn_norm, mlp_norm,
          w_qkv.reshape(layers, d_model, qkv_cols), w_out, w_gate, w_up, w_down,
          k_cache.reshape(layers, rows, seq, head_dim), v_cache.reshape(layers, rows, seq, head_dim))

    cache_spec = P(None, 'dp', None, 'tp', None)
    in_specs = (P('dp', None), P('dp'), cache_spec, cache_spec, P(), P(None, None, 'tp', None),
                P(None, 'tp', None), P(), P(None, None, 'tp'), P(None, None, 'tp'), P(None, 'tp', None))
    return jax.shard_map(local_step, mesh=mesh, in_specs=in_specs, out_specs=P('dp', None), check_vma=False)
```

```python
import functools

import jax
import jax.numpy as jnp
from jax import lax
from jax.experimental import pallas as pl
from jax.experimental.pallas import tpu as pltpu
from jax.sharding import PartitionSpec as P

ROPE_BASE = 10000.0
NORM_EPS = 1e-5
F32 = jnp.float32
BF16 = jnp.bfloat16
MESH = pl.DeviceIdType.MESH
CORES = 2
HALVES = 2
NEG = -1e30


def rope_tables(lengths, head_dim):
    inv_freq = ROPE_BASE ** (-jnp.arange(0, head_dim, 2, dtype=F32) / head_dim)
    angles = lengths.astype(F32)[:, None] * inv_freq[None, :]
    cosine, sine = jnp.cos(angles), jnp.sin(angles)
    return jnp.concatenate([cosine, cosine], 1), jnp.concatenate([-sine, sine], 1)


def kernel(cfg, hid, lens, cos_ref, sin_ref, gain_attn, gain_mlp, wqkv, wout, wgate, wup, wdown, kc, vc, out,
           x, a_buf, rbuf, lrep, part, rel_in, prt_in, dir_in, own_in, f_out, f_in, stat,
           q_s, kn_s, vn_s, s_s, attn, act, g_acc, u_acc, b_g, b_u, b_d, b_v,
           rs_sem, ag_sem, st_sem, snd_sem, snd2_sem, w_sem, k_sem, g_sem, x_sem):
    layers, rows, width, head_dim, group, chips, seq = cfg
    part_rows = rows // HALVES
    quart = part_rows // 2
    wide = CORES * width
    qkv_cols = (group + 2) * head_dim
    heads = group * head_dim
    d_model = chips * wide
    n_dev = chips * CORES
    tp = lax.axis_index('tp')
    e = lax.rem(tp, CORES)
    c = lax.div(tp, CORES)
    other = 1 - e
    right = lax.rem(c + 1, chips)
    left = lax.rem(c + chips - 1, chips)
    far = lax.rem(c + 2, chips)
    in_order = (c, left, right, far)
    out_order = (far, right, left, c)
    ways = (pl.ds(0, quart), pl.ds(quart, quart))

    def half_rows(h):
        return pl.ds(h * part_rows, part_rows)

    def way_rows(h, way):
        return pl.ds(h * part_rows + way * quart, quart)

    def dev(chip, core):
        return {'tp': chip * CORES + core}

    def when(cond, body):
        if cond is True:
            body()
        elif cond is not False:
            pl.when(cond)(body)

    def cols(chip):
        return pl.ds(pl.multiple_of(chip * wide, wide), wide)

    def qkv_at(i):
        return b_d.at[i, 0:wide, 0:qkv_cols]

    def out_at(i):
        return b_d.at[i, wide:wide + heads, :]

    per_block = wide // seq
    lane_blocks = (wide - qkv_cols) // head_dim
    n_blocks = -(-rows // per_block)

    def key_at(j, first_row, n):
        lane = qkv_cols + (j % lane_blocks) * head_dim
        return b_d.at[j // lane_blocks, first_row:first_row + n, lane:lane + head_dim]

    def ld_qkv(l, i):
        return pltpu.make_async_copy(wqkv.at[l, cols(in_order[i]), :], qkv_at(i), w_sem.at[i])

    def ld_out(l, i):
        return pltpu.make_async_copy(wout.at[l, :, cols(out_order[i])], out_at(i), w_sem.at[4 + i])

    def ld_k(l, j):
        n = min(per_block, rows - j * per_block) * seq
        return pltpu.make_async_copy(kc.at[l, pl.ds(j * wide, n), :], key_at(j, 0, n), k_sem.at[j])

    def ld_v(l):
        return pltpu.make_async_copy(vc.at[l], b_v, w_sem.at[12])

    def ld_g(l, i):
        return pltpu.make_async_copy(wgate.at[l, cols(in_order[i]), :], b_g.at[i], g_sem.at[i])

    def ld_u(l, i):
        return pltpu.make_async_copy(wup.at[l, cols(in_order[i]), :], b_u.at[i], g_sem.at[chips + i])

    def ld_d(l, i):
        return pltpu.make_async_copy(wdown.at[l, :, cols(out_order[i])], b_d.at[i], w_sem.at[8 + i])

    def start_keys(l, slots):
        for j in range(n_blocks):
            if j // lane_blocks in slots:
                ld_k(l, j).start()

    x_loads = [pltpu.make_async_copy(
        hid.at[:, pl.ds(k * wide + h * width, width)], x.at[k, h], x_sem.at[k, h])
        for k in range(chips) for h in range(CORES)]
    for cp in x_loads:
        cp.start()
    for i in range(chips):
        ld_qkv(0, i).start()
    start_keys(0, range(chips))
    ld_v(0).start()
    for i in range(chips):
        ld_out(0, i).start()

    barrier = pltpu.get_barrier_semaphore()
    for step in range(1, n_dev):
        pl.semaphore_signal(barrier, inc=1, device_id={'tp': lax.rem(tp + step, n_dev)}, device_id_type=MESH)
    pl.semaphore_wait(barrier, n_dev - 1)

    lens_row = jnp.broadcast_to(lens[...].astype(F32), (rows, rows)).T
    for g in range(group):
        lrep[pl.ds(g, rows, stride=group), :] = lens_row

    for cp in x_loads:
        cp.wait()
    total = jnp.zeros((rows, 128), F32)
    for k in range(chips):
        for h in range(CORES):
            for j in range(width // 128):
                v = x[k, h, :, j * 128:(j + 1) * 128].astype(F32)
                total = total + v * v
    scale0 = lax.rsqrt(jnp.sum(total, axis=1, keepdims=True) / d_model + NORM_EPS)
    rbuf[...] = jnp.broadcast_to(scale0, (rows, 128))

    def normed(chip, gain_ref, l, h):
        r = jnp.concatenate([rbuf[half_rows(h), :]] * (width // 128), axis=1)
        gain = gain_ref[0:1, cols(chip)].astype(F32)
        for k in range(1, layers):
            gain = jnp.where(l == k, gain_ref[k:k + 1, cols(chip)].astype(F32), gain)
        for q in range(CORES):
            piece = x[chip, q, half_rows(h)].astype(F32)
            a_buf[:, q * width:(q + 1) * width] = (
                piece * r * gain[:, q * width:(q + 1) * width]).astype(BF16)

    def accumulate(acc, prod, i):
        if i == 0:
            acc[...] = prod
        else:
            acc[...] += prod

    def use_qkv(l, h):
        def use(i):
            normed(in_order[i], gain_attn, l, h)
            if h == 0:
                ld_qkv(l, i).wait()
            prod = jnp.dot(a_buf[...], qkv_at(i)[...], preferred_element_type=F32)
            accumulate(g_acc.at[:, 0:qkv_cols], prod, i)
        return use

    def use_gu(l, h):
        def use(i):
            normed(in_order[i], gain_mlp, l, h)
            for ld, buf, acc in ((ld_g, b_g, g_acc), (ld_u, b_u, u_acc)):
                if h == 0:
                    ld(l, i).wait()
                accumulate(acc, jnp.dot(a_buf[...], buf[i], preferred_element_type=F32), i)
                if h == 1 and i < 2:
                    when(l + 1 < layers, lambda: ld(l + 1, i).start())
        return use

    def attention(l, h):
        cosine, sine = cos_ref[half_rows(h), :], sin_ref[half_rows(h), :]

        def rot(v):
            return (v * cosine + pltpu.roll(v, head_dim // 2, 1) * sine).astype(BF16).astype(F32)

        def head(j):
            return g_acc[:, j * head_dim:(j + 1) * head_dim].astype(BF16).astype(F32)

        key_new = rot(head(group))
        val_new = head(group + 1)
        for g in range(group):
            at = pl.ds(g, part_rows, stride=group)
            q_s[at, :] = rot(head(g))
            kn_s[at, :] = key_new
            vn_s[at, :] = val_new
        scale = head_dim ** -0.5
        pair = 2 * group
        upper = lax.broadcasted_iota(jnp.int32, (pair, head_dim), 0) < group
        if h == 0:
            for j in range(n_blocks):
                ld_k(l, j).wait()
        for p in range(part_rows // 2):
            at = slice(p * pair, (p + 1) * pair)
            b = h * part_rows + 2 * p
            keys = key_at(b // per_block, b % per_block * seq, 2 * seq)[...]
            s = lax.dot_general(q_s[at, :].astype(BF16), keys, (((1,), (1,)), ((), ())),
                                preferred_element_type=F32)
            s_s[at, :] = jnp.where(upper, s[:, :seq], s[:, seq:])
        pos = lax.broadcasted_iota(jnp.int32, (part_rows * group, seq), 1).astype(F32)
        live = pos < lrep[h * part_rows * group:(h + 1) * part_rows * group, :]
        s = jnp.where(live, s_s[...] * scale, NEG)
        own = jnp.sum(q_s[...] * kn_s[...], axis=1, keepdims=True) * scale
        peak = jnp.maximum(jnp.max(s, axis=1, keepdims=True), own)
        w = jnp.exp(s - peak).astype(BF16).astype(F32)
        w_own = jnp.exp(own - peak).astype(BF16).astype(F32)
        denom = jnp.sum(w, axis=1, keepdims=True) + w_own
        s_s[...] = w
        q_s[...] = w_own * vn_s[...]
        kn_s[...] = jnp.broadcast_to(denom, kn_s.shape)
        if h == 0:
            ld_v(l).wait()
        for p in range(part_rows // 2):
            at = slice(p * pair, (p + 1) * pair)
            b = h * part_rows + 2 * p
            vals = jnp.concatenate([b_v[b], b_v[b + 1]], axis=1)
            o = jnp.dot(s_s[at, :].astype(BF16), vals, preferred_element_type=F32)
            o = jnp.where(upper, o[:, :head_dim], o[:, head_dim:])
            s_s[at, :] = (o + q_s[at, :]) / kn_s[at, :]
        if h == 1:
            when(l + 1 < layers, lambda: ld_v(l + 1).start())
        for g in range(group):
            attn[:, g * head_dim:(g + 1) * head_dim] = s_s[pl.ds(g, part_rows, stride=group), :].astype(BF16)

    def activate():
        gate = g_acc[...].astype(BF16).astype(F32)
        up = u_acc[...].astype(BF16).astype(F32)
        act[...] = (gate * jax.nn.sigmoid(gate) * up).astype(BF16)

    def put_part(h, i, prod):
        part[h, i, 0] = prod[:, :width].astype(BF16)
        part[h, i, 1] = prod[:, width:].astype(BF16)

    def chunk_out(l, h):
        def chunk(i):
            if h == 0:
                ld_out(l, i).wait()
            put_part(h, i, jnp.dot(attn[...], out_at(i)[...], preferred_element_type=F32))
            if h == 1:
                ld_d(l, i).start()
        return chunk

    def chunk_down(l, h):
        def chunk(i):
            if h == 0:
                ld_d(l, i).wait()
            put_part(h, i, jnp.dot(act[...], b_d[i], preferred_element_type=F32))
            if h == 1:
                def nxt():
                    ld_qkv(l + 1, i).start()
                    start_keys(l + 1, (i,))
                    if i == chips - 1:
                        for k in range(chips):
                            ld_out(l + 1, k).start()
                        for k in range(2, chips):
                            ld_g(l + 1, k).start()
                            ld_u(l + 1, k).start()
                when(l + 1 < layers, nxt)
        return chunk

    def remote(src, dst, ssem, rsem, where):
        return pltpu.make_async_remote_copy(
            src_ref=src, dst_ref=dst, send_sem=ssem, recv_sem=rsem, device_id=where, device_id_type=MESH)

    me = dev(c, e)

    def arrived(dst, rsem):
        remote(dst, dst, rsem, rsem, me).wait_recv()

    def sent(src, ssem):
        remote(src, src, ssem, ssem, me).wait_send()

    def scatter_sends(h, i):
        if i == 0:
            return [(part.at[h, 0, q, ways[w]], rel_in.at[h, w, e], rs_sem.at[h, 2 * w + e],
                     dev((right, left)[w], q)) for q in range(CORES) for w in range(2)]
        if i in (1, 2):
            w = i - 1
            hop = (right, left)[w]
            return [(part.at[h, i, other, ways[w]], prt_in.at[h, w], rs_sem.at[h, 4 + w], dev(c, other))] + [
                (part.at[h, i, q, ways[1 - w]], dir_in.at[h, 1 - w, e], rs_sem.at[h, 6 + 2 * (1 - w) + e],
                 dev(hop, q)) for q in range(CORES)]
        if i == 3:
            return [(part.at[h, 3, other], own_in.at[h], rs_sem.at[h, 12], dev(c, other))]
        w = i - 4
        return [(f_out.at[h, w], f_in.at[h, w], rs_sem.at[h, 10 + w], dev((right, left)[w], e))]

    scatter_base = (0, 4, 7, 10, 11, 12)

    def scatter(h, i):
        for n, (src, dst, rsem, where) in enumerate(scatter_sends(h, i)):
            remote(src, dst, snd_sem.at[h, scatter_base[i] + n], rsem, where).start()

    def relay(h):
        for w in range(2):
            for q in range(CORES):
                arrived(rel_in.at[h, w, q], rs_sem.at[h, 2 * w + q])
            arrived(prt_in.at[h, w], rs_sem.at[h, 4 + w])
            f_out[h, w] = (rel_in[h, w, 0].astype(F32) + rel_in[h, w, 1].astype(F32)
                           + (prt_in[h, w].astype(F32) + part[h, 1 + w, e, ways[w]].astype(F32)))
            scatter(h, 4 + w)

    def gather_sends(h, group_id):
        def push(chip, core, w, where):
            ref = x.at[chip, core, way_rows(h, w)]
            return ref, ref, ag_sem.at[h, chip, core, w], where
        mate = dev(c, other)
        if group_id == 0:
            return [(stat.at[h, tp], stat.at[h, tp], st_sem.at[h, tp], {'tp': lax.rem(tp + step, n_dev)})
                    for step in range(1, n_dev)]
        if group_id == 1:
            return [push(c, e, 0, dev(right, e)), push(c, e, 1, dev(left, e)),
                    push(c, e, 1, dev(right, e)), push(c, e, 0, dev(left, e)),
                    push(c, e, 0, mate), push(c, e, 1, mate)]
        if group_id == 2:
            return [push(left, e, 0, dev(right, e)), push(left, e, 0, mate)]
        if group_id == 3:
            return [push(right, e, 1, dev(left, e)), push(right, e, 1, mate)]
        if group_id == 4:
            return [push(left, e, 1, mate)]
        if group_id == 5:
            return [push(right, e, 0, mate)]
        return [push(far, e, 0, mate), push(far, e, 1, mate)]

    gather_base = (0, 7, 13, 15, 17, 18, 19)

    def gather(h, i):
        for n, (src, dst, rsem, where) in enumerate(gather_sends(h, i)):
            remote(src, dst, snd2_sem.at[h, gather_base[i] + n], rsem, where).start()

    def gather_done(h, with_stats):
        for i in range(0 if with_stats else 1, 7):
            for n, (src, dst, rsem, where) in enumerate(gather_sends(h, i)):
                sent(src, snd2_sem.at[h, gather_base[i] + n])

    def have(h, chip, core, w):
        arrived(x.at[chip, core, way_rows(h, w)], ag_sem.at[h, chip, core, w])

    def have_both(h, chip, core):
        have(h, chip, core, 0)
        have(h, chip, core, 1)

    def finish_sum(h, with_stats):
        arrived(own_in.at[h], rs_sem.at[h, 12])
        squares = []
        for w in range(2):
            for q in range(CORES):
                arrived(dir_in.at[h, w, q], rs_sem.at[h, 6 + 2 * w + q])
            arrived(f_in.at[h, w], rs_sem.at[h, 10 + w])
            v = ((part[h, 3, e, ways[w]].astype(F32) + own_in[h, ways[w]].astype(F32))
                 + (dir_in[h, w, 0].astype(F32) + dir_in[h, w, 1].astype(F32)) + f_in[h, w])
            v = (x[c, e, way_rows(h, w)].astype(F32) + v).astype(BF16)
            x[c, e, way_rows(h, w)] = v
            v = v.astype(F32)
            sq = v * v
            tot = sq[:, :128]
            for j in range(1, width // 128):
                tot = tot + sq[:, j * 128:(j + 1) * 128]
            squares.append(tot)
        gather(h, 1)
        if with_stats:
            row = jnp.sum(jnp.concatenate(squares * HALVES, axis=0).T, axis=0, keepdims=True)
            stat[h, tp] = jnp.broadcast_to(row, (8, rows))
            gather(h, 0)
        for i in range(6):
            for n, (src, dst, rsem, where) in enumerate(scatter_sends(h, i)):
                sent(src, snd_sem.at[h, scatter_base[i] + n])

    def forward(h, with_stats):
        have(h, left, e, 0)
        gather(h, 2)
        have(h, right, e, 1)
        gather(h, 3)
        if with_stats:
            for step in range(1, n_dev):
                src = lax.rem(tp + step, n_dev)
                arrived(stat.at[h, src], st_sem.at[h, src])
            row = stat[h, 0, 0:1]
            for j in range(1, n_dev):
                row = row + stat[h, j, 0:1]
            r = jnp.broadcast_to(lax.rsqrt(row / d_model + NORM_EPS), (rows, rows)).T
            rbuf[half_rows(h), :] = r[:part_rows]
        have(h, left, e, 1)
        gather(h, 4)
        have(h, right, e, 0)
        gather(h, 5)
        have_both(h, c, other)

    def forward_far(h):
        have_both(h, far, e)
        gather(h, 6)

    def window(producing, p, chunk, gathered, h, use, finish, next_chunk, with_stats=True,
               sum_stats=True):
        def rest():
            for i in range(1, chips):
                chunk(i)
                scatter(p, i)
        when(producing, rest)
        when(gathered, lambda: forward(h, with_stats))
        use(0)
        when(producing, lambda: relay(p))
        when(gathered, lambda: have_both(h, left, other))
        use(1)

        def mid():
            forward_far(h)
            have_both(h, right, other)
        when(gathered, mid)
        use(2)
        when(gathered, lambda: have_both(h, far, other))
        use(3)
        when(gathered, lambda: gather_done(h, with_stats))
        finish()
        when(producing, lambda: finish_sum(p, sum_stats))
        if next_chunk is not None:
            next_chunk(0)
            scatter(h, 0)

    def layer(l, carry):
        later = l > 0
        window(later, 1, chunk_down(l - 1, 1), later, 0, use_qkv(l, 0), lambda: attention(l, 0), chunk_out(l, 0))

        def first_gu():
            for i in range(chips):
                ld_g(0, i).start()
                ld_u(0, i).start()
        when(l == 0, first_gu)
        window(True, 0, chunk_out(l, 0), later, 1, use_qkv(l, 1), lambda: attention(l, 1), chunk_out(l, 1))
        window(True, 1, chunk_out(l, 1), True, 0, use_gu(l, 0), activate, chunk_down(l, 0))
        window(True, 0, chunk_down(l, 0), True, 1, use_gu(l, 1), activate, chunk_down(l, 1))
        return carry

    lax.fori_loop(0, layers, layer, 0)

    def out_copy(h, i, q):
        return pltpu.make_async_copy(
            x.at[in_order[i], q, half_rows(h)],
            out.at[half_rows(h), pl.ds(pl.multiple_of(in_order[i] * wide + q * width, width), width)],
            g_sem.at[(h * chips + i) * CORES + q])

    def store(h):
        def use(i):
            for q in range(CORES):
                out_copy(h, i, q).start()
        return use

    window(True, 1, chunk_down(layers - 1, 1), True, 0, store(0), lambda: None, None, sum_stats=False)
    window(False, 0, None, True, 1, store(1), lambda: None, None, with_stats=False)
    for h in range(HALVES):
        for i in range(chips):
            for q in range(CORES):
                out_copy(h, i, q).wait()


def solution(mesh):
    n_dev = mesh.shape['tp']
    chips = n_dev // CORES

    def local_step(hidden, lengths, k_cache, v_cache, attn_norm, w_qkv, w_out, mlp_norm, w_gate, w_up, w_down):
        layers, rows, seq, _, head_dim = k_cache.shape
        d_model = hidden.shape[1]
        width = d_model // n_dev
        qkv_cols = w_qkv.shape[3]
        group = qkv_cols // head_dim - 2
        ff = w_gate.shape[2]
        half = rows // HALVES
        quart = half // 2
        wide = CORES * width
        heads = group * head_dim
        cosine, sine = rope_tables(lengths, head_dim)
        cfg = (layers, rows, width, head_dim, group, chips, seq)
        vmem = pl.BlockSpec(memory_space=pltpu.VMEM)
        hbm = pl.BlockSpec(memory_space=pl.ANY)
        flops = 2 * layers * rows * d_model * (qkv_cols + heads + 3 * ff)
        dma = pltpu.SemaphoreType.DMA
        return pl.pallas_call(
            functools.partial(kernel, cfg),
            out_shape=jax.ShapeDtypeStruct((rows, d_model), BF16),
            in_specs=[hbm] + [vmem] * 5 + [hbm] * 7,
            out_specs=hbm,
            scratch_shapes=[
                pltpu.VMEM((chips, CORES, rows, width), BF16),
                pltpu.VMEM((half, wide), BF16),
                pltpu.VMEM((rows, 128), F32),
                pltpu.VMEM((rows * group, seq), F32),
                pltpu.VMEM((HALVES, chips, CORES, half, width), BF16),
                pltpu.VMEM((HALVES, 2, CORES, quart, width), BF16),
                pltpu.VMEM((HALVES, 2, quart, width), BF16),
                pltpu.VMEM((HALVES, 2, CORES, quart, width), BF16),
                pltpu.VMEM((HALVES, half, width), BF16),
                pltpu.VMEM((HALVES, 2, quart, width), F32),
                pltpu.VMEM((HALVES, 2, quart, width), F32),
                pltpu.VMEM((HALVES, n_dev, 8, rows), F32),
                pltpu.VMEM((half * group, head_dim), F32),
                pltpu.VMEM((half * group, head_dim), F32),
                pltpu.VMEM((half * group, head_dim), F32),
                pltpu.VMEM((half * group, seq), F32),
                pltpu.VMEM((half, heads), BF16),
                pltpu.VMEM((half, ff), BF16),
                pltpu.VMEM((half, ff), F32),
                pltpu.VMEM((half, ff), F32),
                pltpu.VMEM((chips, wide, ff), BF16),
                pltpu.VMEM((chips, wide, ff), BF16),
                pltpu.VMEM((chips, ff, wide), BF16),
                pltpu.VMEM((rows, seq, head_dim), BF16),
                dma((HALVES, 13)),
                dma((HALVES, chips, CORES, 2)),
                dma((HALVES, n_dev)),
                dma((HALVES, 13)),
                dma((HALVES, 21)),
                dma((13,)),
                dma((16,)),
                dma((16,)),
                dma((chips, CORES)),
            ],
            compiler_params=pltpu.CompilerParams(
                collective_id=0, has_side_effects=True, vmem_limit_bytes=67043328),
            cost_estimate=pl.CostEstimate(flops=flops, bytes_accessed=flops // rows, transcendentals=0),
        )(hidden, lengths.reshape(1, rows), cosine, sine, attn_norm, mlp_norm,
          w_qkv.reshape(layers, d_model, qkv_cols), w_out, w_gate, w_up, w_down,
          k_cache.reshape(layers, rows * seq, head_dim), v_cache.reshape(layers, rows, seq, head_dim))

    cache_spec = P(None, 'dp', None, 'tp', None)
    in_specs = (P('dp', None), P('dp'), cache_spec, cache_spec, P(), P(None, None, 'tp', None),
                P(None, 'tp', None), P(), P(None, None, 'tp'), P(None, None, 'tp'), P(None, 'tp', None))
    return jax.shard_map(local_step, mesh=mesh, in_specs=in_specs, out_specs=P('dp', None), check_vma=False)
```

```python
import functools

import jax
import jax.numpy as jnp
import numpy as np
from jax import lax
from jax.experimental import pallas as pl
from jax.experimental.pallas import tpu as pltpu
from jax.sharding import PartitionSpec as P

ROPE_BASE = 10000.0
NORM_EPS = 1e-5
F32 = jnp.float32
BF16 = jnp.bfloat16
MESH = pl.DeviceIdType.MESH
CORES = 2
GU_SLOTS = 5
DN_SLOTS = 2
SPLIT = 4
NEG = -1e30


def kernel(cfg, hid, lens, freq, gain_attn, gain_mlp, wqkv, wout, wgate, wup, wdown, kc, vc, out,
           x, a_buf, rbuf, lrep, part, rel_in, prt_in, dir_in, own_in, f_out, f_in, stat, squares, cos_ref, sin_ref,
           q_s, kn_s, vn_s, s_s, attn, act, g_acc, u_acc,
           b_qkv, b_out, b_k, b_v, b_gu, b_d,
           rs_sem, rel_sem, dir_sem, f_sem, ag_sem, st_sem, snd_sem, snd2_sem, w_sem, x_sem):
    layers, rows, width, head_dim, group, chips, seq = cfg
    half = rows // 2
    wide = CORES * width
    qkv_cols = (group + 2) * head_dim
    d_model = chips * wide
    tp = lax.axis_index('tp')
    e = lax.rem(tp, CORES)
    c = lax.div(tp, CORES)
    other = 1 - e
    right = lax.rem(c + 1, chips)
    left = lax.rem(c + chips - 1, chips)
    far = lax.rem(c + 2, chips)
    first = pl.ds(0, half)
    second = pl.ds(half, half)

    def dev(chip, core):
        return {'tp': chip * CORES + core}

    def cols(chip):
        return pl.ds(pl.multiple_of(chip * wide, wide), wide)

    in_order = (c, left, right, far)
    out_order = (far, right, left, c)

    def ld_qkv(l, i):
        return pltpu.make_async_copy(wqkv.at[l, cols(in_order[i]), :], b_qkv.at[i], w_sem.at[i])

    def ld_out(l, i):
        return pltpu.make_async_copy(wout.at[l, :, cols(out_order[i])], b_out.at[i], w_sem.at[4 + i])

    def ld_k(l):
        return pltpu.make_async_copy(kc.at[l], b_k, w_sem.at[8])

    def ld_v(l):
        return pltpu.make_async_copy(vc.at[l], b_v, w_sem.at[9])

    def ld_gu(m):
        l, i, s = m // (2 * chips), m // 2 % chips, m % GU_SLOTS
        src = wup if m % 2 else wgate
        return pltpu.make_async_copy(src.at[l, cols(in_order[i]), :], b_gu.at[s], w_sem.at[10 + s])

    def ld_d(n):
        l, i, s = n // chips, n % chips, n % DN_SLOTS
        return pltpu.make_async_copy(wdown.at[l, :, cols(out_order[i])], b_d.at[s], w_sem.at[10 + GU_SLOTS + s])

    x_loads = [pltpu.make_async_copy(
        hid.at[:, pl.ds(k * wide + h * width, width)], x.at[k, h], x_sem.at[k, h])
        for k in range(chips) for h in range(CORES)]
    for cp in x_loads:
        cp.start()
    for i in range(chips):
        ld_qkv(0, i).start()
    ld_k(0).start()
    ld_v(0).start()
    for i in range(chips):
        ld_out(0, i).start()

    barrier = pltpu.get_barrier_semaphore()
    n_dev = chips * CORES
    for step in range(1, n_dev):
        pl.semaphore_signal(barrier, inc=1, device_id={'tp': lax.rem(tp + step, n_dev)}, device_id_type=MESH)
    pl.semaphore_wait(barrier, n_dev - 1)

    lens_row = jnp.broadcast_to(lens[...].astype(F32), (rows, rows)).T
    for g in range(group):
        lrep[pl.ds(g, rows, stride=group), :] = lens_row
    angles = lens_row[:, :head_dim] * freq[...]
    sine = jnp.sin(angles)
    cos_ref[...] = jnp.cos(angles)
    sin_ref[...] = jnp.where(lax.broadcasted_iota(jnp.int32, angles.shape, 1) < head_dim // 2, -sine, sine)

    for cp in x_loads:
        cp.wait()
    total = jnp.zeros((rows, 128), F32)
    for k in range(chips):
        for h in range(CORES):
            for j in range(width // 128):
                v = x[k, h, :, j * 128:(j + 1) * 128].astype(F32)
                total = total + v * v
    scale0 = lax.rsqrt(jnp.sum(total, axis=1, keepdims=True) / d_model + NORM_EPS)
    rbuf[...] = jnp.broadcast_to(scale0, (rows, 128))

    def normed(chip, gain_ref, l):
        r = jnp.concatenate([rbuf[...]] * (width // 128), axis=1)
        gain = gain_ref[l:l + 1, cols(chip)].astype(F32)
        for h in range(CORES):
            piece = x[chip, h].astype(F32)
            a_buf[:, h * width:(h + 1) * width] = (
                piece * r * gain[:, h * width:(h + 1) * width]).astype(BF16)

    def use_qkv(l):
        def consume(i):
            normed(in_order[i], gain_attn, l)
            ld_qkv(l, i).wait()
            prod = jnp.dot(a_buf[...], b_qkv[i], preferred_element_type=F32)
            if i == 0:
                g_acc[:, :qkv_cols] = prod
            else:
                g_acc[:, :qkv_cols] += prod
            if l + 1 < layers:
                ld_qkv(l + 1, i).start()
        return consume

    def use_gu(l):
        def consume(i):
            normed(in_order[i], gain_mlp, l)
            for j, acc in enumerate((g_acc, u_acc)):
                m = 2 * (l * chips + i) + j
                ld_gu(m).wait()
                prod = jnp.dot(a_buf[...], b_gu[m % GU_SLOTS], preferred_element_type=F32)
                if i == 0:
                    acc[...] = prod
                else:
                    acc[...] += prod
                if m + GU_SLOTS < layers * chips * 2:
                    ld_gu(m + GU_SLOTS).start()
        return consume

    def attention(l):
        cosine, sine = cos_ref[...], sin_ref[...]

        def rot(v):
            return (v * cosine + pltpu.roll(v, head_dim // 2, 1) * sine).astype(BF16).astype(F32)

        def head(j):
            return g_acc[:, j * head_dim:(j + 1) * head_dim].astype(BF16).astype(F32)

        key_new = rot(head(group))
        val_new = head(group + 1)
        for g in range(group):
            at = pl.ds(g, rows, stride=group)
            q_s[at, :] = rot(head(g))
            kn_s[at, :] = key_new
            vn_s[at, :] = val_new
        scale = head_dim ** -0.5
        pair = 2 * group
        upper = lax.broadcasted_iota(jnp.int32, (pair, head_dim), 0) < group
        ld_k(l).wait()

        def scores(i, carry):
            at = pl.ds(pl.multiple_of(i * pair, pair), pair)
            q = q_s[at, :].astype(BF16)
            keys = b_k[pl.ds(i * 2, 2)].reshape(2 * seq, head_dim)
            s = lax.dot_general(q, keys, (((1,), (1,)), ((), ())), preferred_element_type=F32)
            s_s[at, :] = jnp.where(upper, s[:, :seq], s[:, seq:])
            return carry

        lax.fori_loop(0, rows // 2, scores, 0, unroll=8)
        if l + 1 < layers:
            ld_k(l + 1).start()
        pos = lax.broadcasted_iota(jnp.int32, (rows * group, seq), 1).astype(F32)
        s = jnp.where(pos < lrep[...], s_s[...] * scale, NEG)
        own = jnp.sum(q_s[...] * kn_s[...], axis=1, keepdims=True) * scale
        peak = jnp.maximum(jnp.max(s, axis=1, keepdims=True), own)
        w = jnp.exp(s - peak).astype(BF16).astype(F32)
        w_own = jnp.exp(own - peak).astype(BF16).astype(F32)
        denom = jnp.sum(w, axis=1, keepdims=True) + w_own
        s_s[...] = w
        q_s[...] = w_own * vn_s[...]
        kn_s[...] = jnp.broadcast_to(denom, kn_s.shape)
        ld_v(l).wait()

        def mix(i, carry):
            at = pl.ds(pl.multiple_of(i * pair, pair), pair)
            w = s_s[at, :].astype(BF16)
            vals = jnp.concatenate([b_v[i * 2], b_v[i * 2 + 1]], axis=1)
            o = jnp.dot(w, vals, preferred_element_type=F32)
            o = jnp.where(upper, o[:, :head_dim], o[:, head_dim:])
            s_s[at, :] = (o + q_s[at, :]) / kn_s[at, :]
            return carry

        lax.fori_loop(0, rows // 2, mix, 0, unroll=8)
        if l + 1 < layers:
            ld_v(l + 1).start()
        for g in range(group):
            attn[:, g * head_dim:(g + 1) * head_dim] = s_s[pl.ds(g, rows, stride=group), :].astype(BF16)

    def chunk_out(l):
        def chunk(i):
            ld_out(l, i).wait()
            prod = jnp.dot(attn[...], b_out[i], preferred_element_type=F32)
            part[i, 0] = prod[:, :width].astype(BF16)
            part[i, 1] = prod[:, width:].astype(BF16)
            if l + 1 < layers:
                ld_out(l + 1, i).start()
        return chunk

    def chunk_down(l):
        def chunk(i):
            n = l * chips + i
            ld_d(n).wait()
            prod = jnp.dot(act[...], b_d[n % DN_SLOTS], preferred_element_type=F32)
            part[i, 0] = prod[:, :width].astype(BF16)
            part[i, 1] = prod[:, width:].astype(BF16)
            if n + DN_SLOTS < layers * chips:
                ld_d(n + DN_SLOTS).start()
        return chunk

    step_rows = half // SPLIT

    def rows_of(w, s):
        return pl.ds(w * half + s * step_rows, step_rows)

    def remote(src, dst, ssem, rsem, where):
        return pltpu.make_async_remote_copy(
            src_ref=src, dst_ref=dst, send_sem=ssem, recv_sem=rsem, device_id=where, device_id_type=MESH)

    me = dev(c, e)
    mate = dev(c, other)

    def arrived(dst, rsem):
        remote(dst, dst, rsem, rsem, me).wait_recv()

    class Sends:
        def __init__(self, sems):
            self.sems, self.all = sems, []

        def __call__(self, src, dst, rsem, where):
            cp = remote(src, dst, self.sems.at[len(self.all)], rsem, where)
            cp.start()
            self.all.append(cp)

        def done(self):
            for cp in self.all:
                cp.wait_send()

    toward = (right, left)

    def reduce_scatter(chunk, finished):
        send = Sends(snd_sem)

        def piece(s):
            return pl.ds(s * step_rows, step_rows)

        def send_direct(s):
            for q in range(CORES):
                send(part.at[1, q, rows_of(1, s)], dir_in.at[1, e, piece(s)], dir_sem.at[1, e, s], dev(right, q))
                send(part.at[2, q, rows_of(0, s)], dir_in.at[0, e, piece(s)], dir_sem.at[0, e, s], dev(left, q))

        chunk(0)
        for s in range(SPLIT):
            for q in range(CORES):
                for w in range(2):
                    send(part.at[0, q, rows_of(w, s)], rel_in.at[w, e, piece(s)], rel_sem.at[w, e, s],
                         dev(toward[w], q))
        chunk(1)
        send(part.at[1, other, first], prt_in.at[0], rs_sem.at[0], mate)
        chunk(2)
        send(part.at[2, other, second], prt_in.at[1], rs_sem.at[1], mate)
        send_direct(0)
        chunk(3)
        send(part.at[3, other], own_in, rs_sem.at[2], mate)
        for w in range(2):
            arrived(prt_in.at[w], rs_sem.at[w])
        for s in range(SPLIT):
            at = slice(s * step_rows, (s + 1) * step_rows)
            for w in range(2):
                for q in range(CORES):
                    arrived(rel_in.at[w, q, piece(s)], rel_sem.at[w, q, s])
                f_out[w, at] = (rel_in[w, 0, at].astype(F32) + rel_in[w, 1, at].astype(F32)
                                + (prt_in[w, at].astype(F32) + part[1 + w, e, rows_of(w, s)].astype(F32)))
                send(f_out.at[w, piece(s)], f_in.at[w, piece(s)], f_sem.at[w, s], dev(toward[w], e))
            if s + 1 < SPLIT:
                send_direct(s + 1)
        arrived(own_in, rs_sem.at[2])
        for s in range(SPLIT):
            at = slice(s * step_rows, (s + 1) * step_rows)
            for w in range(2):
                where = rows_of(w, s)
                for q in range(CORES):
                    arrived(dir_in.at[w, q, piece(s)], dir_sem.at[w, q, s])
                arrived(f_in.at[w, piece(s)], f_sem.at[w, s])
                v = ((part[3, e, where].astype(F32) + own_in[where].astype(F32))
                     + (dir_in[w, 0, at].astype(F32) + dir_in[w, 1, at].astype(F32)) + f_in[w, at])
                v = (x[c, e, where].astype(F32) + v).astype(BF16)
                x[c, e, where] = v
                v = v.astype(F32)
                sq = v * v
                tot = sq[:, :128]
                for j in range(1, width // 128):
                    tot = tot + sq[:, j * 128:(j + 1) * 128]
                squares[where, :] = tot
            finished(s)
        send.done()

    def reduce(chunk, consume, with_stats=True):
        send = Sends(snd2_sem)

        def push(chip, core, w, s, where):
            ref = x.at[chip, core, rows_of(w, s)]
            send(ref, ref, ag_sem.at[chip, core, w, s], where)

        def have(chip, core, w, s):
            arrived(x.at[chip, core, rows_of(w, s)], ag_sem.at[chip, core, w, s])

        def have_all(chip, core):
            for s in range(SPLIT):
                for w in range(2):
                    have(chip, core, w, s)

        def finished(s):
            if with_stats and s == SPLIT - 1:
                row = jnp.sum(squares[...].T, axis=0, keepdims=True)
                stat[tp] = jnp.broadcast_to(row, (8, rows))
                for step in range(1, n_dev):
                    send(stat.at[tp], stat.at[tp], st_sem.at[tp], {'tp': lax.rem(tp + step, n_dev)})
            push(c, e, 0, s, dev(right, e))
            push(c, e, 1, s, dev(left, e))
            push(c, e, 1, s, dev(right, e))
            push(c, e, 0, s, dev(left, e))
            push(c, e, 0, s, mate)
            push(c, e, 1, s, mate)

        reduce_scatter(chunk, finished)
        for s in range(SPLIT):
            have(left, e, 0, s)
            push(left, e, 0, s, dev(right, e))
            push(left, e, 0, s, mate)
            have(right, e, 1, s)
            push(right, e, 1, s, dev(left, e))
            push(right, e, 1, s, mate)
            have(left, e, 1, s)
            push(left, e, 1, s, mate)
            have(right, e, 0, s)
            push(right, e, 0, s, mate)
        if with_stats:
            for step in range(1, n_dev):
                src = lax.rem(tp + step, n_dev)
                arrived(stat.at[src], st_sem.at[src])
            row = stat[0, 0:1]
            for j in range(1, n_dev):
                row = row + stat[j, 0:1]
            rbuf[...] = jnp.broadcast_to(lax.rsqrt(row / d_model + NORM_EPS), (rows, rows)).T
        have_all(c, other)
        consume(0)
        have_all(left, other)
        consume(1)
        for s in range(SPLIT):
            for w in range(2):
                have(far, e, w, s)
                push(far, e, w, s, mate)
        have_all(right, other)
        consume(2)
        have_all(far, other)
        consume(3)
        send.done()

    for i in range(chips):
        use_qkv(0)(i)
    for m in range(GU_SLOTS):
        ld_gu(m).start()
    for l in range(layers):
        attention(l)
        if l == 0:
            for n in range(DN_SLOTS):
                ld_d(n).start()
        reduce(chunk_out(l), use_gu(l))
        gate = g_acc[...].astype(BF16).astype(F32)
        up = u_acc[...].astype(BF16).astype(F32)
        act[...] = (gate * jax.nn.sigmoid(gate) * up).astype(BF16)
        if l + 1 < layers:
            reduce(chunk_down(l), use_qkv(l + 1))
    stores = []

    def store(i):
        for h in range(CORES):
            cp = pltpu.make_async_copy(
                x.at[in_order[i], h],
                out.at[:, pl.ds(pl.multiple_of(in_order[i] * wide + h * width, width), width)],
                x_sem.at[i, h])
            cp.start()
            stores.append(cp)

    reduce(chunk_down(layers - 1), store, with_stats=False)
    for cp in stores:
        cp.wait()


def emit_kernel(src, dst, buf, in_sem, out_sem):
    n = in_sem.shape[0]
    rows = src.shape[0] // n

    def copy_in(i):
        return pltpu.make_async_copy(src.at[pl.ds(i * rows, rows)], buf.at[pl.ds(i * rows, rows)], in_sem.at[i])

    def copy_out(i):
        return pltpu.make_async_copy(buf.at[pl.ds(i * rows, rows)], dst.at[pl.ds(i * rows, rows)], out_sem.at[i])

    for i in range(n):
        copy_in(i).start()
    for i in range(n):
        copy_in(i).wait()
        copy_out(i).start()
    for i in range(n):
        copy_out(i).wait()


def emit(value):
    hbm = pl.BlockSpec(memory_space=pl.ANY)
    return pl.pallas_call(
        emit_kernel, out_shape=jax.ShapeDtypeStruct(value.shape, value.dtype), in_specs=[hbm], out_specs=hbm,
        scratch_shapes=[pltpu.VMEM(value.shape, value.dtype), pltpu.SemaphoreType.DMA((4,)),
                        pltpu.SemaphoreType.DMA((4,))],
        cost_estimate=pl.CostEstimate(flops=0, bytes_accessed=4 * value.size, transcendentals=0))(value)


def solution(mesh):
    n_dev = mesh.shape['tp']
    chips = n_dev // CORES

    def local_step(hidden, lengths, k_cache, v_cache, attn_norm, w_qkv, w_out, mlp_norm, w_gate, w_up, w_down):
        layers, rows, seq, _, head_dim = k_cache.shape
        d_model = hidden.shape[1]
        width = d_model // n_dev
        qkv_cols = w_qkv.shape[3]
        group = qkv_cols // head_dim - 2
        ff = w_gate.shape[2]
        half = rows // 2
        wide = CORES * width
        heads = group * head_dim
        inv_freq = (ROPE_BASE ** (-np.arange(0, head_dim, 2, dtype=np.float32) / head_dim)).astype(np.float32)
        freq = jnp.asarray(np.concatenate([inv_freq, inv_freq])[None, :])
        cfg = (layers, rows, width, head_dim, group, chips, seq)
        vmem = pl.BlockSpec(memory_space=pltpu.VMEM)
        hbm = pl.BlockSpec(memory_space=pl.ANY)
        flops = 2 * layers * rows * d_model * (qkv_cols + heads + 3 * ff)
        return emit(pl.pallas_call(
            functools.partial(kernel, cfg),
            out_shape=jax.ShapeDtypeStruct((rows, d_model), BF16),
            in_specs=[hbm] + [vmem] * 4 + [hbm] * 7,
            out_specs=hbm,
            scratch_shapes=[
                pltpu.VMEM((chips, CORES, rows, width), BF16),
                pltpu.VMEM((rows, wide), BF16),
                pltpu.VMEM((rows, 128), F32),
                pltpu.VMEM((rows * group, seq), F32),
                pltpu.VMEM((chips, CORES, rows, width), BF16),
                pltpu.VMEM((2, CORES, half, width), BF16),
                pltpu.VMEM((2, half, width), BF16),
                pltpu.VMEM((2, CORES, half, width), BF16),
                pltpu.VMEM((rows, width), BF16),
                pltpu.VMEM((2, half, width), F32),
                pltpu.VMEM((2, half, width), F32),
                pltpu.VMEM((n_dev, 8, rows), F32),
                pltpu.VMEM((rows, 128), F32),
                pltpu.VMEM((rows, head_dim), F32),
                pltpu.VMEM((rows, head_dim), F32),
                pltpu.VMEM((rows * group, head_dim), F32),
                pltpu.VMEM((rows * group, head_dim), F32),
                pltpu.VMEM((rows * group, head_dim), F32),
                pltpu.VMEM((rows * group, seq), F32),
                pltpu.VMEM((rows, heads), BF16),
                pltpu.VMEM((rows, ff), BF16),
                pltpu.VMEM((rows, ff), F32),
                pltpu.VMEM((rows, ff), F32),
                pltpu.VMEM((chips, wide, qkv_cols), BF16),
                pltpu.VMEM((chips, heads, wide), BF16),
                pltpu.VMEM((rows, seq, head_dim), BF16),
                pltpu.VMEM((rows, seq, head_dim), BF16),
                pltpu.VMEM((GU_SLOTS, wide, ff), BF16),
                pltpu.VMEM((DN_SLOTS, ff, wide), BF16),
                pltpu.SemaphoreType.DMA((3,)),
                pltpu.SemaphoreType.DMA((2, CORES, SPLIT)),
                pltpu.SemaphoreType.DMA((2, CORES, SPLIT)),
                pltpu.SemaphoreType.DMA((2, SPLIT)),
                pltpu.SemaphoreType.DMA((chips, CORES, 2, SPLIT)),
                pltpu.SemaphoreType.DMA((n_dev,)),
                pltpu.SemaphoreType.DMA((3 + 10 * SPLIT,)),
                pltpu.SemaphoreType.DMA((n_dev - 1 + 14 * SPLIT,)),
                pltpu.SemaphoreType.DMA((10 + GU_SLOTS + DN_SLOTS,)),
                pltpu.SemaphoreType.DMA((chips, CORES)),
            ],
            compiler_params=pltpu.CompilerParams(
                collective_id=0, has_side_effects=True, vmem_limit_bytes=67043328),
            cost_estimate=pl.CostEstimate(flops=flops, bytes_accessed=flops // rows, transcendentals=0),
        )(hidden, lengths.reshape(1, rows), freq, attn_norm, mlp_norm,
          w_qkv.reshape(layers, d_model, qkv_cols), w_out, w_gate, w_up, w_down,
          k_cache.reshape(layers, rows, seq, head_dim), v_cache.reshape(layers, rows, seq, head_dim)))

    cache_spec = P(None, 'dp', None, 'tp', None)
    in_specs = (P('dp', None), P('dp'), cache_spec, cache_spec, P(), P(None, None, 'tp', None),
                P(None, 'tp', None), P(), P(None, None, 'tp'), P(None, None, 'tp'), P(None, 'tp', None))
    return jax.shard_map(local_step, mesh=mesh, in_specs=in_specs, out_specs=P('dp', None), check_vma=False)
```

```python
import functools

import jax
import jax.numpy as jnp
import numpy as np
from jax import lax
from jax.experimental import pallas as pl
from jax.experimental.pallas import tpu as pltpu
from jax.sharding import PartitionSpec as P

ROPE_BASE = 10000.0
NORM_EPS = 1e-5
F32 = jnp.float32
BF16 = jnp.bfloat16
MESH = pl.DeviceIdType.MESH
CORES = 2
GU_SLOTS = 7
SPLIT = 4
NEG = -1e30


def kernel(cfg, hid, lens, freq, gain_attn, gain_mlp, wqkv, wout, wgate, wup, wdown, kc, vc, out,
           x, a_buf, rbuf, lrep, part, rel_in, prt_in, dir_in, own_in, f_out, f_in, stat, squares, cos_ref, sin_ref,
           q_s, kn_s, vn_s, s_s, attn, act, g_acc, u_acc,
           b_v, b_gu, b_d,
           rs_sem, rel_sem, dir_sem, f_sem, ag_sem, st_sem, snd_sem, snd2_sem, w_sem, k_sem, g_sem, x_sem):
    layers, rows, width, head_dim, group, chips, seq = cfg
    half = rows // 2
    wide = CORES * width
    qkv_cols = (group + 2) * head_dim
    heads = group * head_dim
    d_model = chips * wide
    tp = lax.axis_index('tp')
    e = lax.rem(tp, CORES)
    c = lax.div(tp, CORES)
    other = 1 - e
    right = lax.rem(c + 1, chips)
    left = lax.rem(c + chips - 1, chips)
    far = lax.rem(c + 2, chips)
    first = pl.ds(0, half)
    second = pl.ds(half, half)

    def dev(chip, core):
        return {'tp': chip * CORES + core}

    def cols(chip):
        return pl.ds(pl.multiple_of(chip * wide, wide), wide)

    in_order = (c, left, right, far)
    out_order = (far, right, left, c)

    def qkv_at(i):
        return b_d.at[i, 0:wide, 0:qkv_cols]

    def out_at(i):
        return b_d.at[i, wide:wide + heads, :]

    per_block = wide // seq
    lane_blocks = (wide - qkv_cols) // head_dim
    n_blocks = -(-rows // per_block)
    full_blocks = rows // per_block

    def keys_at(j, first_row, n):
        lane = pl.multiple_of(qkv_cols + (j % lane_blocks) * head_dim, head_dim)
        return b_d.at[j // lane_blocks, pl.ds(first_row, n), pl.ds(lane, head_dim)]

    def ld_qkv(l, i):
        return pltpu.make_async_copy(wqkv.at[l, cols(in_order[i]), :], qkv_at(i), w_sem.at[i])

    def ld_out(l, i):
        return pltpu.make_async_copy(wout.at[l, :, cols(out_order[i])], out_at(i), w_sem.at[4 + i])

    def ld_k(l, j):
        n = min(per_block, rows - j * per_block) * seq
        return pltpu.make_async_copy(kc.at[l, pl.ds(j * wide, n), :], keys_at(j, 0, n), k_sem.at[j])

    def ld_v(l):
        return pltpu.make_async_copy(vc.at[l], b_v, w_sem.at[8])

    def ld_gu(m):
        l, i, s = m // (2 * chips), m // 2 % chips, m % GU_SLOTS
        src = wup if m % 2 else wgate
        return pltpu.make_async_copy(src.at[l, cols(in_order[i]), :], b_gu.at[s], g_sem.at[s])

    def ld_d(l, i):
        return pltpu.make_async_copy(wdown.at[l, :, cols(out_order[i])], b_d.at[i], w_sem.at[9 + i])

    x_loads = [pltpu.make_async_copy(
        hid.at[:, pl.ds(k * wide + h * width, width)], x.at[k, h], x_sem.at[k, h])
        for k in range(chips) for h in range(CORES)]
    for cp in x_loads:
        cp.start()
    for i in range(chips):
        ld_qkv(0, i).start()
    for j in range(n_blocks):
        ld_k(0, j).start()
    ld_v(0).start()
    for i in range(chips):
        ld_out(0, i).start()

    barrier = pltpu.get_barrier_semaphore()
    n_dev = chips * CORES
    for step in range(1, n_dev):
        pl.semaphore_signal(barrier, inc=1, device_id={'tp': lax.rem(tp + step, n_dev)}, device_id_type=MESH)
    pl.semaphore_wait(barrier, n_dev - 1)

    lens_row = jnp.broadcast_to(lens[...].astype(F32), (rows, rows)).T
    for g in range(group):
        lrep[pl.ds(g, rows, stride=group), :] = lens_row
    angles = lens_row[:, :head_dim] * freq[...]
    sine = jnp.sin(angles)
    cos_ref[...] = jnp.cos(angles)
    sin_ref[...] = jnp.where(lax.broadcasted_iota(jnp.int32, angles.shape, 1) < head_dim // 2, -sine, sine)

    for cp in x_loads:
        cp.wait()
    total = jnp.zeros((rows, 128), F32)
    for k in range(chips):
        for h in range(CORES):
            for j in range(width // 128):
                v = x[k, h, :, j * 128:(j + 1) * 128].astype(F32)
                total = total + v * v
    scale0 = lax.rsqrt(jnp.sum(total, axis=1, keepdims=True) / d_model + NORM_EPS)
    rbuf[...] = jnp.broadcast_to(scale0, (rows, 128))

    def normed(chip, gain_ref, l):
        r = jnp.concatenate([rbuf[...]] * (width // 128), axis=1)
        gain = gain_ref[l:l + 1, cols(chip)].astype(F32)
        for h in range(CORES):
            piece = x[chip, h].astype(F32)
            a_buf[:, h * width:(h + 1) * width] = (
                piece * r * gain[:, h * width:(h + 1) * width]).astype(BF16)

    def use_qkv(l):
        def consume(i):
            normed(in_order[i], gain_attn, l)
            ld_qkv(l, i).wait()
            prod = jnp.dot(a_buf[...], qkv_at(i)[...], preferred_element_type=F32)
            if i == 0:
                g_acc[:, :qkv_cols] = prod
            else:
                g_acc[:, :qkv_cols] += prod
        return consume

    def use_gu(l):
        def consume(i):
            normed(in_order[i], gain_mlp, l)
            for j, acc in enumerate((g_acc, u_acc)):
                m = 2 * (l * chips + i) + j
                ld_gu(m).wait()
                prod = jnp.dot(a_buf[...], b_gu[m % GU_SLOTS], preferred_element_type=F32)
                if i == 0:
                    acc[...] = prod
                else:
                    acc[...] += prod
                if m + GU_SLOTS < layers * chips * 2:
                    ld_gu(m + GU_SLOTS).start()
        return consume

    def attention(l):
        cosine, sine = cos_ref[...], sin_ref[...]

        def rot(v):
            return (v * cosine + pltpu.roll(v, head_dim // 2, 1) * sine).astype(BF16).astype(F32)

        def head(j):
            return g_acc[:, j * head_dim:(j + 1) * head_dim].astype(BF16).astype(F32)

        key_new = rot(head(group))
        val_new = head(group + 1)
        for g in range(group):
            at = pl.ds(g, rows, stride=group)
            q_s[at, :] = rot(head(g))
            kn_s[at, :] = key_new
            vn_s[at, :] = val_new
        scale = head_dim ** -0.5
        pair = 2 * group
        upper = lax.broadcasted_iota(jnp.int32, (pair, head_dim), 0) < group
        for j in range(n_blocks):
            ld_k(l, j).wait()

        def score(j, p):
            at = pl.ds(pl.multiple_of((j * (per_block // 2) + p) * pair, pair), pair)
            keys = keys_at(j, p * 2 * seq, 2 * seq)[...]
            s = lax.dot_general(q_s[at, :].astype(BF16), keys, (((1,), (1,)), ((), ())),
                                preferred_element_type=F32)
            s_s[at, :] = jnp.where(upper, s[:, :seq], s[:, seq:])

        def scores(j, carry):
            for p in range(per_block // 2):
                score(j, p)
            return carry

        lax.fori_loop(0, full_blocks, scores, 0)
        for p in range((rows - full_blocks * per_block) // 2):
            score(full_blocks, p)
        pos = lax.broadcasted_iota(jnp.int32, (rows * group, seq), 1).astype(F32)
        s = jnp.where(pos < lrep[...], s_s[...] * scale, NEG)
        own = jnp.sum(q_s[...] * kn_s[...], axis=1, keepdims=True) * scale
        peak = jnp.maximum(jnp.max(s, axis=1, keepdims=True), own)
        w = jnp.exp(s - peak).astype(BF16).astype(F32)
        w_own = jnp.exp(own - peak).astype(BF16).astype(F32)
        denom = jnp.sum(w, axis=1, keepdims=True) + w_own
        s_s[...] = w
        q_s[...] = w_own * vn_s[...]
        kn_s[...] = jnp.broadcast_to(denom, kn_s.shape)
        ld_v(l).wait()

        def mix(i, carry):
            at = pl.ds(pl.multiple_of(i * pair, pair), pair)
            w = s_s[at, :].astype(BF16)
            vals = jnp.concatenate([b_v[i * 2], b_v[i * 2 + 1]], axis=1)
            o = jnp.dot(w, vals, preferred_element_type=F32)
            o = jnp.where(upper, o[:, :head_dim], o[:, head_dim:])
            s_s[at, :] = (o + q_s[at, :]) / kn_s[at, :]
            return carry

        lax.fori_loop(0, rows // 2, mix, 0, unroll=8)
        if l + 1 < layers:
            ld_v(l + 1).start()
        for g in range(group):
            attn[:, g * head_dim:(g + 1) * head_dim] = s_s[pl.ds(g, rows, stride=group), :].astype(BF16)

    def chunk_out(l):
        def chunk(i):
            ld_out(l, i).wait()
            prod = jnp.dot(attn[...], out_at(i)[...], preferred_element_type=F32)
            part[i, 0] = prod[:, :width].astype(BF16)
            part[i, 1] = prod[:, width:].astype(BF16)
            ld_d(l, i).start()
        return chunk

    def chunk_down(l):
        def chunk(i):
            ld_d(l, i).wait()
            prod = jnp.dot(act[...], b_d[i], preferred_element_type=F32)
            part[i, 0] = prod[:, :width].astype(BF16)
            part[i, 1] = prod[:, width:].astype(BF16)
            if l + 1 < layers:
                ld_qkv(l + 1, i).start()
                for j in range(n_blocks):
                    if j // lane_blocks == i:
                        ld_k(l + 1, j).start()
                if i == chips - 1:
                    for k in range(chips):
                        ld_out(l + 1, k).start()
        return chunk

    step_rows = half // SPLIT

    def rows_of(w, s):
        return pl.ds(w * half + s * step_rows, step_rows)

    def remote(src, dst, ssem, rsem, where):
        return pltpu.make_async_remote_copy(
            src_ref=src, dst_ref=dst, send_sem=ssem, recv_sem=rsem, device_id=where, device_id_type=MESH)

    me = dev(c, e)
    mate = dev(c, other)

    def arrived(dst, rsem):
        remote(dst, dst, rsem, rsem, me).wait_recv()

    class Sends:
        def __init__(self, sems):
            self.sems, self.all = sems, []

        def __call__(self, src, dst, rsem, where):
            cp = remote(src, dst, self.sems.at[len(self.all)], rsem, where)
            cp.start()
            self.all.append(cp)

        def done(self):
            for cp in self.all:
                cp.wait_send()

    toward = (right, left)

    def reduce_scatter(chunk, finished):
        send = Sends(snd_sem)

        def piece(s):
            return pl.ds(s * step_rows, step_rows)

        def send_direct(s):
            for q in range(CORES):
                send(part.at[1, q, rows_of(1, s)], dir_in.at[1, e, piece(s)], dir_sem.at[1, e, s], dev(right, q))
                send(part.at[2, q, rows_of(0, s)], dir_in.at[0, e, piece(s)], dir_sem.at[0, e, s], dev(left, q))

        chunk(0)
        for s in range(SPLIT):
            for q in range(CORES):
                for w in range(2):
                    send(part.at[0, q, rows_of(w, s)], rel_in.at[w, e, piece(s)], rel_sem.at[w, e, s],
                         dev(toward[w], q))
        chunk(1)
        send(part.at[1, other, first], prt_in.at[0], rs_sem.at[0], mate)
        chunk(2)
        send(part.at[2, other, second], prt_in.at[1], rs_sem.at[1], mate)
        send_direct(0)
        chunk(3)
        send(part.at[3, other], own_in, rs_sem.at[2], mate)
        for w in range(2):
            arrived(prt_in.at[w], rs_sem.at[w])
        for s in range(SPLIT):
            at = slice(s * step_rows, (s + 1) * step_rows)
            for w in range(2):
                for q in range(CORES):
                    arrived(rel_in.at[w, q, piece(s)], rel_sem.at[w, q, s])
                f_out[w, at] = (rel_in[w, 0, at].astype(F32) + rel_in[w, 1, at].astype(F32)
                                + (prt_in[w, at].astype(F32) + part[1 + w, e, rows_of(w, s)].astype(F32)))
                send(f_out.at[w, piece(s)], f_in.at[w, piece(s)], f_sem.at[w, s], dev(toward[w], e))
            if s + 1 < SPLIT:
                send_direct(s + 1)
        arrived(own_in, rs_sem.at[2])
        for s in range(SPLIT):
            at = slice(s * step_rows, (s + 1) * step_rows)
            for w in range(2):
                where = rows_of(w, s)
                for q in range(CORES):
                    arrived(dir_in.at[w, q, piece(s)], dir_sem.at[w, q, s])
                arrived(f_in.at[w, piece(s)], f_sem.at[w, s])
                v = ((part[3, e, where].astype(F32) + own_in[where].astype(F32))
                     + (dir_in[w, 0, at].astype(F32) + dir_in[w, 1, at].astype(F32)) + f_in[w, at])
                v = (x[c, e, where].astype(F32) + v).astype(BF16)
                x[c, e, where] = v
                v = v.astype(F32)
                sq = v * v
                tot = sq[:, :128]
                for j in range(1, width // 128):
                    tot = tot + sq[:, j * 128:(j + 1) * 128]
                squares[where, :] = tot
            finished(s)
        send.done()

    def reduce(chunk, consume, with_stats=True):
        send = Sends(snd2_sem)

        def push(chip, core, w, s, where):
            ref = x.at[chip, core, rows_of(w, s)]
            send(ref, ref, ag_sem.at[chip, core, w, s], where)

        def have(chip, core, w, s):
            arrived(x.at[chip, core, rows_of(w, s)], ag_sem.at[chip, core, w, s])

        def have_all(chip, core):
            for s in range(SPLIT):
                for w in range(2):
                    have(chip, core, w, s)

        def finished(s):
            if with_stats and s == SPLIT - 1:
                row = jnp.sum(squares[...].T, axis=0, keepdims=True)
                stat[tp] = jnp.broadcast_to(row, (8, rows))
                for step in range(1, n_dev):
                    send(stat.at[tp], stat.at[tp], st_sem.at[tp], {'tp': lax.rem(tp + step, n_dev)})
            push(c, e, 0, s, dev(right, e))
            push(c, e, 1, s, dev(left, e))
            push(c, e, 1, s, dev(right, e))
            push(c, e, 0, s, dev(left, e))
            push(c, e, 0, s, mate)
            push(c, e, 1, s, mate)

        reduce_scatter(chunk, finished)
        for s in range(SPLIT):
            have(left, e, 0, s)
            push(left, e, 0, s, dev(right, e))
            push(left, e, 0, s, mate)
            have(right, e, 1, s)
            push(right, e, 1, s, dev(left, e))
            push(right, e, 1, s, mate)
            have(left, e, 1, s)
            push(left, e, 1, s, mate)
            have(right, e, 0, s)
            push(right, e, 0, s, mate)
        if with_stats:
            for step in range(1, n_dev):
                src = lax.rem(tp + step, n_dev)
                arrived(stat.at[src], st_sem.at[src])
            row = stat[0, 0:1]
            for j in range(1, n_dev):
                row = row + stat[j, 0:1]
            rbuf[...] = jnp.broadcast_to(lax.rsqrt(row / d_model + NORM_EPS), (rows, rows)).T
        have_all(c, other)
        consume(0)
        have_all(left, other)
        consume(1)
        for s in range(SPLIT):
            for w in range(2):
                have(far, e, w, s)
                push(far, e, w, s, mate)
        have_all(right, other)
        consume(2)
        have_all(far, other)
        consume(3)
        send.done()

    for i in range(chips):
        use_qkv(0)(i)
    for m in range(GU_SLOTS):
        ld_gu(m).start()
    for l in range(layers):
        attention(l)
        reduce(chunk_out(l), use_gu(l))
        gate = g_acc[...].astype(BF16).astype(F32)
        up = u_acc[...].astype(BF16).astype(F32)
        act[...] = (gate * jax.nn.sigmoid(gate) * up).astype(BF16)
        if l + 1 < layers:
            reduce(chunk_down(l), use_qkv(l + 1))
    stores = []

    def store(i):
        for h in range(CORES):
            cp = pltpu.make_async_copy(
                x.at[in_order[i], h],
                out.at[:, pl.ds(pl.multiple_of(in_order[i] * wide + h * width, width), width)],
                x_sem.at[i, h])
            cp.start()
            stores.append(cp)

    reduce(chunk_down(layers - 1), store, with_stats=False)
    for cp in stores:
        cp.wait()


def emit_kernel(src, dst, buf, in_sem, out_sem):
    n = in_sem.shape[0]
    rows = src.shape[0] // n

    def copy_in(i):
        return pltpu.make_async_copy(src.at[pl.ds(i * rows, rows)], buf.at[pl.ds(i * rows, rows)], in_sem.at[i])

    def copy_out(i):
        return pltpu.make_async_copy(buf.at[pl.ds(i * rows, rows)], dst.at[pl.ds(i * rows, rows)], out_sem.at[i])

    for i in range(n):
        copy_in(i).start()
    for i in range(n):
        copy_in(i).wait()
        copy_out(i).start()
    for i in range(n):
        copy_out(i).wait()


def emit(value):
    hbm = pl.BlockSpec(memory_space=pl.ANY)
    return pl.pallas_call(
        emit_kernel, out_shape=jax.ShapeDtypeStruct(value.shape, value.dtype), in_specs=[hbm], out_specs=hbm,
        scratch_shapes=[pltpu.VMEM(value.shape, value.dtype), pltpu.SemaphoreType.DMA((4,)),
                        pltpu.SemaphoreType.DMA((4,))],
        cost_estimate=pl.CostEstimate(flops=0, bytes_accessed=4 * value.size, transcendentals=0))(value)


def solution(mesh):
    n_dev = mesh.shape['tp']
    chips = n_dev // CORES

    def local_step(hidden, lengths, k_cache, v_cache, attn_norm, w_qkv, w_out, mlp_norm, w_gate, w_up, w_down):
        layers, rows, seq, _, head_dim = k_cache.shape
        d_model = hidden.shape[1]
        width = d_model // n_dev
        qkv_cols = w_qkv.shape[3]
        group = qkv_cols // head_dim - 2
        ff = w_gate.shape[2]
        half = rows // 2
        wide = CORES * width
        heads = group * head_dim
        inv_freq = (ROPE_BASE ** (-np.arange(0, head_dim, 2, dtype=np.float32) / head_dim)).astype(np.float32)
        freq = jnp.asarray(np.concatenate([inv_freq, inv_freq])[None, :])
        cfg = (layers, rows, width, head_dim, group, chips, seq)
        vmem = pl.BlockSpec(memory_space=pltpu.VMEM)
        hbm = pl.BlockSpec(memory_space=pl.ANY)
        flops = 2 * layers * rows * d_model * (qkv_cols + heads + 3 * ff)
        return emit(pl.pallas_call(
            functools.partial(kernel, cfg),
            out_shape=jax.ShapeDtypeStruct((rows, d_model), BF16),
            in_specs=[hbm] + [vmem] * 4 + [hbm] * 7,
            out_specs=hbm,
            scratch_shapes=[
                pltpu.VMEM((chips, CORES, rows, width), BF16),
                pltpu.VMEM((rows, wide), BF16),
                pltpu.VMEM((rows, 128), F32),
                pltpu.VMEM((rows * group, seq), F32),
                pltpu.VMEM((chips, CORES, rows, width), BF16),
                pltpu.VMEM((2, CORES, half, width), BF16),
                pltpu.VMEM((2, half, width), BF16),
                pltpu.VMEM((2, CORES, half, width), BF16),
                pltpu.VMEM((rows, width), BF16),
                pltpu.VMEM((2, half, width), F32),
                pltpu.VMEM((2, half, width), F32),
                pltpu.VMEM((n_dev, 8, rows), F32),
                pltpu.VMEM((rows, 128), F32),
                pltpu.VMEM((rows, head_dim), F32),
                pltpu.VMEM((rows, head_dim), F32),
                pltpu.VMEM((rows * group, head_dim), F32),
                pltpu.VMEM((rows * group, head_dim), F32),
                pltpu.VMEM((rows * group, head_dim), F32),
                pltpu.VMEM((rows * group, seq), F32),
                pltpu.VMEM((rows, heads), BF16),
                pltpu.VMEM((rows, ff), BF16),
                pltpu.VMEM((rows, ff), F32),
                pltpu.VMEM((rows, ff), F32),
                pltpu.VMEM((rows, seq, head_dim), BF16),
                pltpu.VMEM((GU_SLOTS, wide, ff), BF16),
                pltpu.VMEM((chips, ff, wide), BF16),
                pltpu.SemaphoreType.DMA((3,)),
                pltpu.SemaphoreType.DMA((2, CORES, SPLIT)),
                pltpu.SemaphoreType.DMA((2, CORES, SPLIT)),
                pltpu.SemaphoreType.DMA((2, SPLIT)),
                pltpu.SemaphoreType.DMA((chips, CORES, 2, SPLIT)),
                pltpu.SemaphoreType.DMA((n_dev,)),
                pltpu.SemaphoreType.DMA((3 + 10 * SPLIT,)),
                pltpu.SemaphoreType.DMA((n_dev - 1 + 14 * SPLIT,)),
                pltpu.SemaphoreType.DMA((13,)),
                pltpu.SemaphoreType.DMA((16,)),
                pltpu.SemaphoreType.DMA((GU_SLOTS,)),
                pltpu.SemaphoreType.DMA((chips, CORES)),
            ],
            compiler_params=pltpu.CompilerParams(
                collective_id=0, has_side_effects=True, vmem_limit_bytes=67043328),
            cost_estimate=pl.CostEstimate(flops=flops, bytes_accessed=flops // rows, transcendentals=0),
        )(hidden, lengths.reshape(1, rows), freq, attn_norm, mlp_norm,
          w_qkv.reshape(layers, d_model, qkv_cols), w_out, w_gate, w_up, w_down,
          k_cache.reshape(layers, rows * seq, head_dim), v_cache.reshape(layers, rows, seq, head_dim)))

    cache_spec = P(None, 'dp', None, 'tp', None)
    in_specs = (P('dp', None), P('dp'), cache_spec, cache_spec, P(), P(None, None, 'tp', None),
                P(None, 'tp', None), P(), P(None, None, 'tp'), P(None, None, 'tp'), P(None, 'tp', None))
    return jax.shard_map(local_step, mesh=mesh, in_specs=in_specs, out_specs=P('dp', None), check_vma=False)
```

```python
import functools

import jax
import jax.numpy as jnp
import numpy as np
from jax import lax
from jax.experimental import pallas as pl
from jax.experimental.pallas import tpu as pltpu
from jax.sharding import PartitionSpec as P

ROPE_BASE = 10000.0
NORM_EPS = 1e-5
F32 = jnp.float32
BF16 = jnp.bfloat16
MESH = pl.DeviceIdType.MESH
CORES = 2
GU_SLOTS = 7
SPLIT = 4
V_PARTS = 8
NEG = -1e30


def kernel(cfg, hid, lens, freq, gain_attn, gain_mlp, wqkv, wout, wgate, wup, wdown, kc, vc, out,
           x, a_buf, rbuf, lrep, part, rel_in, prt_in, dir_in, own_in, f_out, f_in, stat, squares, cos_ref, sin_ref,
           q_s, kn_s, vn_s, s_s, attn, act, g_acc, u_acc,
           b_v, b_gu, b_d,
           rs_sem, rel_sem, dir_sem, f_sem, ag_sem, mate_sem, st_sem, snd_sem, snd2_sem, w_sem, k_sem, v_sem, g_sem, x_sem):
    layers, rows, width, head_dim, group, chips, seq = cfg
    half = rows // 2
    wide = CORES * width
    qkv_cols = (group + 2) * head_dim
    heads = group * head_dim
    d_model = chips * wide
    tp = lax.axis_index('tp')
    e = lax.rem(tp, CORES)
    c = lax.div(tp, CORES)
    other = 1 - e
    right = lax.rem(c + 1, chips)
    left = lax.rem(c + chips - 1, chips)
    far = lax.rem(c + 2, chips)
    first = pl.ds(0, half)
    second = pl.ds(half, half)

    def dev(chip, core):
        return {'tp': chip * CORES + core}

    def cols(chip):
        return pl.ds(pl.multiple_of(chip * wide, wide), wide)

    in_order = (c, left, right, far)
    out_order = (far, right, left, c)

    def qkv_at(i):
        return b_d.at[i, 0:wide, 0:qkv_cols]

    def out_at(i):
        return b_d.at[i, wide:wide + heads, :]

    per_block = wide // seq
    lane_blocks = (wide - qkv_cols) // head_dim
    n_blocks = -(-rows // per_block)
    full_blocks = rows // per_block

    def keys_at(j, first_row, n):
        lane = pl.multiple_of(qkv_cols + (j % lane_blocks) * head_dim, head_dim)
        return b_d.at[j // lane_blocks, pl.ds(first_row, n), pl.ds(lane, head_dim)]

    def ld_qkv(l, i):
        return pltpu.make_async_copy(wqkv.at[l, cols(in_order[i]), :], qkv_at(i), w_sem.at[i])

    def ld_out(l, i):
        return pltpu.make_async_copy(wout.at[l, :, cols(out_order[i])], out_at(i), w_sem.at[4 + i])

    def ld_k(l, j):
        n = (per_block if not isinstance(j, int) or j < full_blocks else rows - j * per_block) * seq
        return pltpu.make_async_copy(kc.at[l, pl.ds(j * wide, n), :], keys_at(j, 0, n), k_sem.at[j])

    v_rows = rows // V_PARTS

    def ld_v(l, i):
        at = pl.ds(i * v_rows, v_rows)
        return pltpu.make_async_copy(vc.at[l, at], b_v.at[at], v_sem.at[i])

    def ld_gu(m):
        l, i, s = m // (2 * chips), m // 2 % chips, m % GU_SLOTS
        src = wup if m % 2 else wgate
        return pltpu.make_async_copy(src.at[l, cols(in_order[i]), :], b_gu.at[s], g_sem.at[s])

    def ld_d(l, i):
        return pltpu.make_async_copy(wdown.at[l, :, cols(out_order[i])], b_d.at[i], w_sem.at[9 + i])

    x_loads = [pltpu.make_async_copy(
        hid.at[:, pl.ds(k * wide + h * width, width)], x.at[k, h], x_sem.at[k, h])
        for k in range(chips) for h in range(CORES)]
    for cp in x_loads:
        cp.start()
    for i in range(chips):
        ld_qkv(0, i).start()
    for j in range(n_blocks):
        ld_k(0, j).start()
    for i in range(V_PARTS):
        ld_v(0, i).start()
    for i in range(chips):
        ld_out(0, i).start()

    barrier = pltpu.get_barrier_semaphore()
    n_dev = chips * CORES
    for step in range(1, n_dev):
        pl.semaphore_signal(barrier, inc=1, device_id={'tp': lax.rem(tp + step, n_dev)}, device_id_type=MESH)
    pl.semaphore_wait(barrier, n_dev - 1)

    lens_row = jnp.broadcast_to(lens[...].astype(F32), (rows, rows)).T
    for g in range(group):
        lrep[pl.ds(g, rows, stride=group), :] = lens_row
    angles = lens_row[:, :head_dim] * freq[...]
    sine = jnp.sin(angles)
    cos_ref[...] = jnp.cos(angles)
    sin_ref[...] = jnp.where(lax.broadcasted_iota(jnp.int32, angles.shape, 1) < head_dim // 2, -sine, sine)

    for cp in x_loads:
        cp.wait()
    total = jnp.zeros((rows, 128), F32)
    for k in range(chips):
        for h in range(CORES):
            for j in range(width // 128):
                v = x[k, h, :, j * 128:(j + 1) * 128].astype(F32)
                total = total + v * v
    scale0 = lax.rsqrt(jnp.sum(total, axis=1, keepdims=True) / d_model + NORM_EPS)
    rbuf[...] = jnp.broadcast_to(scale0, (rows, 128))

    def normed(chip, gain_ref, l, q):
        r = jnp.concatenate([rbuf[...]] * (width // 128), axis=1)
        at = pl.ds(pl.multiple_of(chip * wide + q * width, width), width)
        gain = gain_ref[l:l + 1, at].astype(F32)
        return (x[chip, q].astype(F32) * r * gain).astype(BF16)

    def take(i, q, gain_ref, l):
        if q is None:
            for k in range(CORES):
                a_buf[:, k * width:(k + 1) * width] = normed(in_order[i], gain_ref, l, k)
            return a_buf, pl.ds(0, wide)
        a_buf[:, 0:width] = normed(in_order[i], gain_ref, l, q)
        return a_buf.at[:, 0:width], pl.ds(pl.multiple_of(q * width, width), width)

    def use_qkv(l):
        def consume(i, q=None):
            a, at = take(i, q, gain_attn, l)
            if q is not other:
                ld_qkv(l, i).wait()
            prod = jnp.dot(a[...], qkv_at(i).at[at, :][...], preferred_element_type=F32)
            if i == 0:
                g_acc[:, :qkv_cols] = prod
            else:
                g_acc[:, :qkv_cols] += prod
        return consume

    def use_gu(l):
        def consume(i, q=None):
            a, at = take(i, q, gain_mlp, l)
            for j, acc in enumerate((g_acc, u_acc)):
                m = 2 * (l * chips + i) + j
                if q is not other:
                    ld_gu(m).wait()
                prod = jnp.dot(a[...], b_gu[m % GU_SLOTS, at, :], preferred_element_type=F32)
                if i == 0:
                    acc[...] = prod
                else:
                    acc[...] += prod
                if q is not e and m + GU_SLOTS < layers * chips * 2:
                    ld_gu(m + GU_SLOTS).start()
        return consume

    def attention(l):
        cosine, sine = cos_ref[...], sin_ref[...]

        def rot(v):
            return (v * cosine + pltpu.roll(v, head_dim // 2, 1) * sine).astype(BF16).astype(F32)

        def head(j):
            return g_acc[:, j * head_dim:(j + 1) * head_dim].astype(BF16).astype(F32)

        key_new = rot(head(group))
        val_new = head(group + 1)
        for g in range(group):
            at = pl.ds(g, rows, stride=group)
            q_s[at, :] = rot(head(g))
            kn_s[at, :] = key_new
            vn_s[at, :] = val_new
        scale = head_dim ** -0.5
        pair = 2 * group
        upper = lax.broadcasted_iota(jnp.int32, (pair, head_dim), 0) < group
        def score(j, p):
            at = pl.ds(pl.multiple_of((j * (per_block // 2) + p) * pair, pair), pair)
            keys = keys_at(j, p * 2 * seq, 2 * seq)[...]
            s = lax.dot_general(q_s[at, :].astype(BF16), keys, (((1,), (1,)), ((), ())),
                                preferred_element_type=F32)
            s_s[at, :] = jnp.where(upper, s[:, :seq], s[:, seq:])

        def scores(j, carry):
            ld_k(l, j).wait()
            for p in range(per_block // 2):
                score(j, p)
            return carry

        lax.fori_loop(0, full_blocks, scores, 0)
        if full_blocks < n_blocks:
            ld_k(l, full_blocks).wait()
        for p in range((rows - full_blocks * per_block) // 2):
            score(full_blocks, p)
        pos = lax.broadcasted_iota(jnp.int32, (rows * group, seq), 1).astype(F32)
        s = jnp.where(pos < lrep[...], s_s[...] * scale, NEG)
        own = jnp.sum(q_s[...] * kn_s[...], axis=1, keepdims=True) * scale
        peak = jnp.maximum(jnp.max(s, axis=1, keepdims=True), own)
        w = jnp.exp(s - peak).astype(BF16).astype(F32)
        w_own = jnp.exp(own - peak).astype(BF16).astype(F32)
        denom = jnp.sum(w, axis=1, keepdims=True) + w_own
        s_s[...] = w
        q_s[...] = w_own * vn_s[...]
        kn_s[...] = jnp.broadcast_to(denom, kn_s.shape)

        def mix(i, carry):
            ld_v(l, i).wait()
            for p in range(v_rows // 2):
                n = i * (v_rows // 2) + p
                at = pl.ds(pl.multiple_of(n * pair, pair), pair)
                w = s_s[at, :].astype(BF16)
                vals = jnp.concatenate([b_v[n * 2], b_v[n * 2 + 1]], axis=1)
                o = jnp.dot(w, vals, preferred_element_type=F32)
                o = jnp.where(upper, o[:, :head_dim], o[:, head_dim:])
                s_s[at, :] = (o + q_s[at, :]) / kn_s[at, :]
            return carry

        lax.fori_loop(0, V_PARTS, mix, 0)
        if l + 1 < layers:
            for i in range(V_PARTS):
                ld_v(l + 1, i).start()
        for g in range(group):
            attn[:, g * head_dim:(g + 1) * head_dim] = s_s[pl.ds(g, rows, stride=group), :].astype(BF16)

    def chunk_out(l):
        def chunk(i):
            ld_out(l, i).wait()
            prod = jnp.dot(attn[...], out_at(i)[...], preferred_element_type=F32)
            part[i, 0] = prod[:, :width].astype(BF16)
            part[i, 1] = prod[:, width:].astype(BF16)
            ld_d(l, i).start()
        return chunk

    def chunk_down(l):
        def chunk(i):
            ld_d(l, i).wait()
            prod = jnp.dot(act[...], b_d[i], preferred_element_type=F32)
            part[i, 0] = prod[:, :width].astype(BF16)
            part[i, 1] = prod[:, width:].astype(BF16)
            if l + 1 < layers:
                ld_qkv(l + 1, i).start()
                for j in range(n_blocks):
                    if j // lane_blocks == i:
                        ld_k(l + 1, j).start()
                if i == chips - 1:
                    for k in range(chips):
                        ld_out(l + 1, k).start()
        return chunk

    step_rows = half // SPLIT

    def rows_of(w, s):
        return pl.ds(w * half + s * step_rows, step_rows)

    def remote(src, dst, ssem, rsem, where):
        return pltpu.make_async_remote_copy(
            src_ref=src, dst_ref=dst, send_sem=ssem, recv_sem=rsem, device_id=where, device_id_type=MESH)

    me = dev(c, e)
    mate = dev(c, other)

    def arrived(dst, rsem):
        remote(dst, dst, rsem, rsem, me).wait_recv()

    class Sends:
        def __init__(self, sems):
            self.sems, self.all = sems, []

        def __call__(self, src, dst, rsem, where):
            cp = remote(src, dst, self.sems.at[len(self.all)], rsem, where)
            cp.start()
            self.all.append(cp)

        def done(self):
            for cp in self.all:
                cp.wait_send()

    toward = (right, left)

    def reduce_scatter(chunk, finished):
        send = Sends(snd_sem)

        def piece(s):
            return pl.ds(s * step_rows, step_rows)

        def send_direct(s):
            for q in range(CORES):
                send(part.at[1, q, rows_of(1, s)], dir_in.at[1, e, piece(s)], dir_sem.at[1, e, s], dev(right, q))
                send(part.at[2, q, rows_of(0, s)], dir_in.at[0, e, piece(s)], dir_sem.at[0, e, s], dev(left, q))

        chunk(0)
        for s in range(SPLIT):
            for q in range(CORES):
                for w in range(2):
                    send(part.at[0, q, rows_of(w, s)], rel_in.at[w, e, piece(s)], rel_sem.at[w, e, s],
                         dev(toward[w], q))
        chunk(1)
        send(part.at[1, other, first], prt_in.at[0], rs_sem.at[0], mate)
        chunk(2)
        send(part.at[2, other, second], prt_in.at[1], rs_sem.at[1], mate)
        send_direct(0)
        chunk(3)
        send(part.at[3, other], own_in, rs_sem.at[2], mate)
        for w in range(2):
            arrived(prt_in.at[w], rs_sem.at[w])
        for s in range(SPLIT):
            at = slice(s * step_rows, (s + 1) * step_rows)
            for w in range(2):
                for q in range(CORES):
                    arrived(rel_in.at[w, q, piece(s)], rel_sem.at[w, q, s])
                f_out[w, at] = (rel_in[w, 0, at].astype(F32) + rel_in[w, 1, at].astype(F32)
                                + (prt_in[w, at].astype(F32) + part[1 + w, e, rows_of(w, s)].astype(F32)))
                send(f_out.at[w, piece(s)], f_in.at[w, piece(s)], f_sem.at[w, s], dev(toward[w], e))
            if s + 1 < SPLIT:
                send_direct(s + 1)
        arrived(own_in, rs_sem.at[2])
        for s in range(SPLIT):
            at = slice(s * step_rows, (s + 1) * step_rows)
            for w in range(2):
                where = rows_of(w, s)
                for q in range(CORES):
                    arrived(dir_in.at[w, q, piece(s)], dir_sem.at[w, q, s])
                arrived(f_in.at[w, piece(s)], f_sem.at[w, s])
                v = ((part[3, e, where].astype(F32) + own_in[where].astype(F32))
                     + (dir_in[w, 0, at].astype(F32) + dir_in[w, 1, at].astype(F32)) + f_in[w, at])
                v = (x[c, e, where].astype(F32) + v).astype(BF16)
                x[c, e, where] = v
                v = v.astype(F32)
                sq = v * v
                tot = sq[:, :128]
                for j in range(1, width // 128):
                    tot = tot + sq[:, j * 128:(j + 1) * 128]
                squares[where, :] = tot
            finished(s)
        send.done()

    def reduce(chunk, consume, with_stats=True):
        send = Sends(snd2_sem)

        def push(chip, core, w, s, where):
            ref = x.at[chip, core, rows_of(w, s)]
            send(ref, ref, ag_sem.at[chip, core, w, s], where)

        def have(chip, core, w, s):
            arrived(x.at[chip, core, rows_of(w, s)], ag_sem.at[chip, core, w, s])

        def share(chip):
            ref = x.at[chip, e]
            send(ref, ref, mate_sem.at[chip], mate)

        def shared(chip):
            arrived(x.at[chip, other], mate_sem.at[chip])

        def finished(s):
            push(c, e, 0, s, dev(right, e))
            push(c, e, 1, s, dev(left, e))
            if with_stats and s == SPLIT - 1:
                row = jnp.sum(squares[...].T, axis=0, keepdims=True)
                stat[tp] = jnp.broadcast_to(row, (8, rows))
                for step in range(1, n_dev):
                    send(stat.at[tp], stat.at[tp], st_sem.at[tp], {'tp': lax.rem(tp + step, n_dev)})
            push(c, e, 1, s, dev(right, e))
            push(c, e, 0, s, dev(left, e))
            if s == SPLIT - 1:
                share(c)

        reduce_scatter(chunk, finished)
        for s in range(SPLIT):
            have(left, e, 0, s)
            push(left, e, 0, s, dev(right, e))
            have(right, e, 1, s)
            push(right, e, 1, s, dev(left, e))
        for s in range(SPLIT):
            have(left, e, 1, s)
        share(left)
        for s in range(SPLIT):
            have(right, e, 0, s)
        share(right)
        if with_stats:
            for step in range(1, n_dev):
                src = lax.rem(tp + step, n_dev)
                arrived(stat.at[src], st_sem.at[src])
            row = stat[0, 0:1]
            for j in range(1, n_dev):
                row = row + stat[j, 0:1]
            rbuf[...] = jnp.broadcast_to(lax.rsqrt(row / d_model + NORM_EPS), (rows, rows)).T
        shared(c)
        consume(0)
        shared(left)
        consume(1)
        for s in range(SPLIT):
            for w in range(2):
                have(far, e, w, s)
        share(far)
        shared(right)
        consume(2)
        consume(3, e)
        shared(far)
        consume(3, other)
        send.done()

    for i in range(chips):
        use_qkv(0)(i)
    for m in range(GU_SLOTS):
        ld_gu(m).start()
    for l in range(layers):
        attention(l)
        reduce(chunk_out(l), use_gu(l))
        gate = g_acc[...].astype(BF16).astype(F32)
        up = u_acc[...].astype(BF16).astype(F32)
        act[...] = (gate * jax.nn.sigmoid(gate) * up).astype(BF16)
        if l + 1 < layers:
            reduce(chunk_down(l), use_qkv(l + 1))
    stores = []

    def store(i, q=None):
        if q is not None and q is e:
            return
        for h in range(CORES):
            cp = pltpu.make_async_copy(
                x.at[in_order[i], h],
                out.at[:, pl.ds(pl.multiple_of(in_order[i] * wide + h * width, width), width)],
                x_sem.at[i, h])
            cp.start()
            stores.append(cp)

    reduce(chunk_down(layers - 1), store, with_stats=False)
    for cp in stores:
        cp.wait()


def emit_kernel(src, dst, buf, in_sem, out_sem):
    n = in_sem.shape[0]
    rows = src.shape[0] // n

    def copy_in(i):
        return pltpu.make_async_copy(src.at[pl.ds(i * rows, rows)], buf.at[pl.ds(i * rows, rows)], in_sem.at[i])

    def copy_out(i):
        return pltpu.make_async_copy(buf.at[pl.ds(i * rows, rows)], dst.at[pl.ds(i * rows, rows)], out_sem.at[i])

    for i in range(n):
        copy_in(i).start()
    for i in range(n):
        copy_in(i).wait()
        copy_out(i).start()
    for i in range(n):
        copy_out(i).wait()


def emit(value):
    hbm = pl.BlockSpec(memory_space=pl.ANY)
    return pl.pallas_call(
        emit_kernel, out_shape=jax.ShapeDtypeStruct(value.shape, value.dtype), in_specs=[hbm], out_specs=hbm,
        scratch_shapes=[pltpu.VMEM(value.shape, value.dtype), pltpu.SemaphoreType.DMA((8,)),
                        pltpu.SemaphoreType.DMA((8,))],
        cost_estimate=pl.CostEstimate(flops=0, bytes_accessed=4 * value.size, transcendentals=0))(value)


def solution(mesh):
    n_dev = mesh.shape['tp']
    chips = n_dev // CORES

    def local_step(hidden, lengths, k_cache, v_cache, attn_norm, w_qkv, w_out, mlp_norm, w_gate, w_up, w_down):
        layers, rows, seq, _, head_dim = k_cache.shape
        d_model = hidden.shape[1]
        width = d_model // n_dev
        qkv_cols = w_qkv.shape[3]
        group = qkv_cols // head_dim - 2
        ff = w_gate.shape[2]
        half = rows // 2
        wide = CORES * width
        heads = group * head_dim
        inv_freq = (ROPE_BASE ** (-np.arange(0, head_dim, 2, dtype=np.float32) / head_dim)).astype(np.float32)
        freq = jnp.asarray(np.concatenate([inv_freq, inv_freq])[None, :])
        cfg = (layers, rows, width, head_dim, group, chips, seq)
        vmem = pl.BlockSpec(memory_space=pltpu.VMEM)
        hbm = pl.BlockSpec(memory_space=pl.ANY)
        flops = 2 * layers * rows * d_model * (qkv_cols + heads + 3 * ff)
        return emit(pl.pallas_call(
            functools.partial(kernel, cfg),
            out_shape=jax.ShapeDtypeStruct((rows, d_model), BF16),
            in_specs=[hbm] + [vmem] * 4 + [hbm] * 7,
            out_specs=hbm,
            scratch_shapes=[
                pltpu.VMEM((chips, CORES, rows, width), BF16),
                pltpu.VMEM((rows, wide), BF16),
                pltpu.VMEM((rows, 128), F32),
                pltpu.VMEM((rows * group, seq), F32),
                pltpu.VMEM((chips, CORES, rows, width), BF16),
                pltpu.VMEM((2, CORES, half, width), BF16),
                pltpu.VMEM((2, half, width), BF16),
                pltpu.VMEM((2, CORES, half, width), BF16),
                pltpu.VMEM((rows, width), BF16),
                pltpu.VMEM((2, half, width), F32),
                pltpu.VMEM((2, half, width), F32),
                pltpu.VMEM((n_dev, 8, rows), F32),
                pltpu.VMEM((rows, 128), F32),
                pltpu.VMEM((rows, head_dim), F32),
                pltpu.VMEM((rows, head_dim), F32),
                pltpu.VMEM((rows * group, head_dim), F32),
                pltpu.VMEM((rows * group, head_dim), F32),
                pltpu.VMEM((rows * group, head_dim), F32),
                pltpu.VMEM((rows * group, seq), F32),
                pltpu.VMEM((rows, heads), BF16),
                pltpu.VMEM((rows, ff), BF16),
                pltpu.VMEM((rows, ff), F32),
                pltpu.VMEM((rows, ff), F32),
                pltpu.VMEM((rows, seq, head_dim), BF16),
                pltpu.VMEM((GU_SLOTS, wide, ff), BF16),
                pltpu.VMEM((chips, ff, wide), BF16),
                pltpu.SemaphoreType.DMA((3,)),
                pltpu.SemaphoreType.DMA((2, CORES, SPLIT)),
                pltpu.SemaphoreType.DMA((2, CORES, SPLIT)),
                pltpu.SemaphoreType.DMA((2, SPLIT)),
                pltpu.SemaphoreType.DMA((chips, CORES, 2, SPLIT)),
                pltpu.SemaphoreType.DMA((chips,)),
                pltpu.SemaphoreType.DMA((n_dev,)),
                pltpu.SemaphoreType.DMA((3 + 10 * SPLIT,)),
                pltpu.SemaphoreType.DMA((n_dev + 3 + 6 * SPLIT,)),
                pltpu.SemaphoreType.DMA((13,)),
                pltpu.SemaphoreType.DMA((16,)),
                pltpu.SemaphoreType.DMA((V_PARTS,)),
                pltpu.SemaphoreType.DMA((GU_SLOTS,)),
                pltpu.SemaphoreType.DMA((chips, CORES)),
            ],
            compiler_params=pltpu.CompilerParams(
                collective_id=0, has_side_effects=True, vmem_limit_bytes=67043328),
            cost_estimate=pl.CostEstimate(flops=flops, bytes_accessed=flops // rows, transcendentals=0),
        )(hidden, lengths.reshape(1, rows), freq, attn_norm, mlp_norm,
          w_qkv.reshape(layers, d_model, qkv_cols), w_out, w_gate, w_up, w_down,
          k_cache.reshape(layers, rows * seq, head_dim), v_cache.reshape(layers, rows, seq, head_dim)))

    cache_spec = P(None, 'dp', None, 'tp', None)
    in_specs = (P('dp', None), P('dp'), cache_spec, cache_spec, P(), P(None, None, 'tp', None),
                P(None, 'tp', None), P(), P(None, None, 'tp'), P(None, None, 'tp'), P(None, 'tp', None))
    return jax.shard_map(local_step, mesh=mesh, in_specs=in_specs, out_specs=P('dp', None), check_vma=False)
```

```python
import functools

import jax
import jax.numpy as jnp
import numpy as np
from jax import lax
from jax.experimental import pallas as pl
from jax.experimental.pallas import tpu as pltpu
from jax.sharding import PartitionSpec as P

ROPE_BASE = 10000.0
NORM_EPS = 1e-5
F32 = jnp.float32
BF16 = jnp.bfloat16
MESH = pl.DeviceIdType.MESH
CORES = 2
GU_SLOTS = 7
SPLIT = 4
V_PARTS = 4
NEG = -1e30


def kernel(cfg, hid, lens, freq, gain_attn, gain_mlp, wqkv, wout, wgate, wup, wdown, kc, vc, out,
           x, a_buf, rbuf, lrep, part, rel_in, prt_in, dir_in, own_in, f_out, f_in, stat, squares, cos_ref, sin_ref,
           q_s, kn_s, vn_s, s_s, attn, act, g_acc, u_acc,
           b_v, b_gu, b_d,
           rs_sem, rel_sem, dir_sem, f_sem, ag_sem, mate_sem, st_sem, snd_sem, snd2_sem, w_sem, k_sem, v_sem, g_sem, x_sem):
    layers, rows, width, head_dim, group, chips, seq = cfg
    half = rows // 2
    wide = CORES * width
    qkv_cols = (group + 2) * head_dim
    heads = group * head_dim
    d_model = chips * wide
    tp = lax.axis_index('tp')
    e = lax.rem(tp, CORES)
    c = lax.div(tp, CORES)
    other = 1 - e
    right = lax.rem(c + 1, chips)
    left = lax.rem(c + chips - 1, chips)
    far = lax.rem(c + 2, chips)
    first = pl.ds(0, half)
    second = pl.ds(half, half)

    def dev(chip, core):
        return {'tp': chip * CORES + core}

    def cols(chip):
        return pl.ds(pl.multiple_of(chip * wide, wide), wide)

    in_order = (c, left, right, far)
    out_order = (far, right, left, c)

    def qkv_at(i):
        return b_d.at[i, 0:wide, 0:qkv_cols]

    def out_at(i):
        return b_d.at[i, wide:wide + heads, :]

    per_block = wide // seq
    lane_blocks = (wide - qkv_cols) // head_dim
    n_blocks = -(-rows // per_block)
    full_blocks = rows // per_block

    def keys_at(j, first_row, n):
        lane = pl.multiple_of(qkv_cols + (j % lane_blocks) * head_dim, head_dim)
        return b_d.at[j // lane_blocks, pl.ds(first_row, n), pl.ds(lane, head_dim)]

    def ld_qkv(l, i):
        return pltpu.make_async_copy(wqkv.at[l, cols(in_order[i]), :], qkv_at(i), w_sem.at[i])

    def ld_out(l, i):
        return pltpu.make_async_copy(wout.at[l, :, cols(out_order[i])], out_at(i), w_sem.at[4 + i])

    def ld_k(l, j):
        n = (per_block if not isinstance(j, int) or j < full_blocks else rows - j * per_block) * seq
        return pltpu.make_async_copy(kc.at[l, pl.ds(j * wide, n), :], keys_at(j, 0, n), k_sem.at[j])

    v_rows = rows // V_PARTS

    def ld_v(l, i):
        at = pl.ds(i * v_rows, v_rows)
        return pltpu.make_async_copy(vc.at[l, at], b_v.at[at], v_sem.at[i])

    def ld_gu(m):
        l, i, s = m // (2 * chips), m // 2 % chips, m % GU_SLOTS
        src = wup if m % 2 else wgate
        return pltpu.make_async_copy(src.at[l, cols(in_order[i]), :], b_gu.at[s], g_sem.at[s])

    def ld_d(l, i):
        return pltpu.make_async_copy(wdown.at[l, :, cols(out_order[i])], b_d.at[i], w_sem.at[9 + i])

    x_loads = [pltpu.make_async_copy(
        hid.at[:, pl.ds(k * wide + h * width, width)], x.at[k, h], x_sem.at[k, h])
        for k in range(chips) for h in range(CORES)]
    for cp in x_loads:
        cp.start()
    for i in range(chips):
        ld_qkv(0, i).start()
    for j in range(n_blocks):
        ld_k(0, j).start()
    for i in range(V_PARTS):
        ld_v(0, i).start()
    for i in range(chips):
        ld_out(0, i).start()

    barrier = pltpu.get_barrier_semaphore()
    n_dev = chips * CORES
    for step in range(1, n_dev):
        pl.semaphore_signal(barrier, inc=1, device_id={'tp': lax.rem(tp + step, n_dev)}, device_id_type=MESH)
    pl.semaphore_wait(barrier, n_dev - 1)

    lens_row = jnp.broadcast_to(lens[...].astype(F32), (rows, rows)).T
    for g in range(group):
        lrep[pl.ds(g, rows, stride=group), :] = lens_row
    angles = lens_row[:, :head_dim] * freq[...]
    sine = jnp.sin(angles)
    cos_ref[...] = jnp.cos(angles)
    sin_ref[...] = jnp.where(lax.broadcasted_iota(jnp.int32, angles.shape, 1) < head_dim // 2, -sine, sine)

    for cp in x_loads:
        cp.wait()
    total = jnp.zeros((rows, 128), F32)
    for k in range(chips):
        for h in range(CORES):
            for j in range(width // 128):
                v = x[k, h, :, j * 128:(j + 1) * 128].astype(F32)
                total = total + v * v
    scale0 = lax.rsqrt(jnp.sum(total, axis=1, keepdims=True) / d_model + NORM_EPS)
    rbuf[...] = jnp.broadcast_to(scale0, (rows, 128))

    def normed(chip, gain_ref, l, q):
        r = jnp.concatenate([rbuf[...]] * (width // 128), axis=1)
        at = pl.ds(pl.multiple_of(chip * wide + q * width, width), width)
        gain = gain_ref[l:l + 1, at].astype(F32)
        return (x[chip, q].astype(F32) * r * gain).astype(BF16)

    def take(i, q, gain_ref, l):
        if q is None:
            for k in range(CORES):
                a_buf[:, k * width:(k + 1) * width] = normed(in_order[i], gain_ref, l, k)
            return a_buf, pl.ds(0, wide)
        a_buf[:, 0:width] = normed(in_order[i], gain_ref, l, q)
        return a_buf.at[:, 0:width], pl.ds(pl.multiple_of(q * width, width), width)

    def use_qkv(l):
        def consume(i, q=None):
            a, at = take(i, q, gain_attn, l)
            if q is not other:
                ld_qkv(l, i).wait()
            prod = jnp.dot(a[...], qkv_at(i).at[at, :][...], preferred_element_type=F32)
            if i == 0:
                g_acc[:, :qkv_cols] = prod
            else:
                g_acc[:, :qkv_cols] += prod
        return consume

    def use_gu(l):
        def consume(i, q=None):
            a, at = take(i, q, gain_mlp, l)
            for j, acc in enumerate((g_acc, u_acc)):
                m = 2 * (l * chips + i) + j
                if q is not other:
                    ld_gu(m).wait()
                prod = jnp.dot(a[...], b_gu[m % GU_SLOTS, at, :], preferred_element_type=F32)
                if i == 0:
                    acc[...] = prod
                else:
                    acc[...] += prod
                if q is not e and m + GU_SLOTS < layers * chips * 2:
                    ld_gu(m + GU_SLOTS).start()
        return consume

    def attention(l):
        cosine, sine = cos_ref[...], sin_ref[...]

        def rot(v):
            return (v * cosine + pltpu.roll(v, head_dim // 2, 1) * sine).astype(BF16).astype(F32)

        def head(j):
            return g_acc[:, j * head_dim:(j + 1) * head_dim].astype(BF16).astype(F32)

        key_new = rot(head(group))
        val_new = head(group + 1)
        for g in range(group):
            at = pl.ds(g, rows, stride=group)
            q_s[at, :] = rot(head(g))
            kn_s[at, :] = key_new
            vn_s[at, :] = val_new
        scale = head_dim ** -0.5
        pair = 2 * group
        upper = lax.broadcasted_iota(jnp.int32, (pair, head_dim), 0) < group
        def score(j, p):
            at = pl.ds(pl.multiple_of((j * (per_block // 2) + p) * pair, pair), pair)
            keys = keys_at(j, p * 2 * seq, 2 * seq)[...]
            s = lax.dot_general(q_s[at, :].astype(BF16), keys, (((1,), (1,)), ((), ())),
                                preferred_element_type=F32)
            s_s[at, :] = jnp.where(upper, s[:, :seq], s[:, seq:])

        def scores(n, carry):
            for k in range(2):
                ld_k(l, n * 2 + k).wait()
            for k in range(2):
                for p in range(per_block // 2):
                    score(n * 2 + k, p)
            return carry

        lax.fori_loop(0, full_blocks // 2, scores, 0)
        for j in range(full_blocks // 2 * 2, full_blocks):
            ld_k(l, j).wait()
            for p in range(per_block // 2):
                score(j, p)
        if full_blocks < n_blocks:
            ld_k(l, full_blocks).wait()
        for p in range((rows - full_blocks * per_block) // 2):
            score(full_blocks, p)
        pos = lax.broadcasted_iota(jnp.int32, (rows * group, seq), 1).astype(F32)
        s = jnp.where(pos < lrep[...], s_s[...] * scale, NEG)
        own = jnp.sum(q_s[...] * kn_s[...], axis=1, keepdims=True) * scale
        peak = jnp.maximum(jnp.max(s, axis=1, keepdims=True), own)
        w = jnp.exp(s - peak).astype(BF16).astype(F32)
        w_own = jnp.exp(own - peak).astype(BF16).astype(F32)
        denom = jnp.sum(w, axis=1, keepdims=True) + w_own
        s_s[...] = w
        q_s[...] = w_own * vn_s[...]
        kn_s[...] = jnp.broadcast_to(denom, kn_s.shape)

        def mix(i, carry):
            ld_v(l, i).wait()
            for p in range(v_rows // 2):
                n = i * (v_rows // 2) + p
                at = pl.ds(pl.multiple_of(n * pair, pair), pair)
                w = s_s[at, :].astype(BF16)
                vals = jnp.concatenate([b_v[n * 2], b_v[n * 2 + 1]], axis=1)
                o = jnp.dot(w, vals, preferred_element_type=F32)
                o = jnp.where(upper, o[:, :head_dim], o[:, head_dim:])
                s_s[at, :] = (o + q_s[at, :]) / kn_s[at, :]
            return carry

        lax.fori_loop(0, V_PARTS, mix, 0)
        if l + 1 < layers:
            for i in range(V_PARTS):
                ld_v(l + 1, i).start()
        for g in range(group):
            attn[:, g * head_dim:(g + 1) * head_dim] = s_s[pl.ds(g, rows, stride=group), :].astype(BF16)

    def multiply(a, w, i, sent):
        if sent is None:
            prod = jnp.dot(a[...], w[...], preferred_element_type=F32)
            part[i, 0] = prod[:, :width].astype(BF16)
            part[i, 1] = prod[:, width:].astype(BF16)
            return
        for q in range(CORES):
            part[i, q] = jnp.dot(a[...], w[:, q * width:(q + 1) * width], preferred_element_type=F32).astype(BF16)
            sent(q)

    def chunk_out(l):
        def chunk(i, sent=None):
            ld_out(l, i).wait()
            multiply(attn, out_at(i), i, sent)
            ld_d(l, i).start()
        return chunk

    def chunk_down(l):
        def chunk(i, sent=None):
            ld_d(l, i).wait()
            multiply(act, b_d.at[i], i, sent)
            if l + 1 < layers:
                ld_qkv(l + 1, i).start()
                for j in range(n_blocks):
                    if j // lane_blocks == i:
                        ld_k(l + 1, j).start()
                if i == chips - 1:
                    for k in range(chips):
                        ld_out(l + 1, k).start()
        return chunk

    step_rows = half // SPLIT

    def rows_of(w, s):
        return pl.ds(w * half + s * step_rows, step_rows)

    def remote(src, dst, ssem, rsem, where):
        return pltpu.make_async_remote_copy(
            src_ref=src, dst_ref=dst, send_sem=ssem, recv_sem=rsem, device_id=where, device_id_type=MESH)

    me = dev(c, e)
    mate = dev(c, other)

    def arrived(dst, rsem):
        remote(dst, dst, rsem, rsem, me).wait_recv()

    class Sends:
        def __init__(self, sems):
            self.sems, self.all = sems, []

        def __call__(self, src, dst, rsem, where):
            cp = remote(src, dst, self.sems.at[len(self.all)], rsem, where)
            cp.start()
            self.all.append(cp)

        def done(self):
            for cp in self.all:
                cp.wait_send()

    toward = (right, left)

    def reduce_scatter(chunk, finished):
        send = Sends(snd_sem)

        def piece(s):
            return pl.ds(s * step_rows, step_rows)

        def send_direct(s):
            for q in range(CORES):
                send(part.at[1, q, rows_of(1, s)], dir_in.at[1, e, piece(s)], dir_sem.at[1, e, s], dev(right, q))
                send(part.at[2, q, rows_of(0, s)], dir_in.at[0, e, piece(s)], dir_sem.at[0, e, s], dev(left, q))

        def send_far(q):
            for s in range(SPLIT):
                for w in range(2):
                    send(part.at[0, q, rows_of(w, s)], rel_in.at[w, e, piece(s)], rel_sem.at[w, e, s],
                         dev(toward[w], q))

        chunk(0, send_far)
        chunk(1)
        send(part.at[1, other, first], prt_in.at[0], rs_sem.at[0], mate)
        chunk(2)
        send(part.at[2, other, second], prt_in.at[1], rs_sem.at[1], mate)
        send_direct(0)
        chunk(3)
        send(part.at[3, other], own_in, rs_sem.at[2], mate)
        for w in range(2):
            arrived(prt_in.at[w], rs_sem.at[w])
        for s in range(SPLIT):
            at = slice(s * step_rows, (s + 1) * step_rows)
            for w in range(2):
                for q in range(CORES):
                    arrived(rel_in.at[w, q, piece(s)], rel_sem.at[w, q, s])
                f_out[w, at] = (rel_in[w, 0, at].astype(F32) + rel_in[w, 1, at].astype(F32)
                                + (prt_in[w, at].astype(F32) + part[1 + w, e, rows_of(w, s)].astype(F32)))
                send(f_out.at[w, piece(s)], f_in.at[w, piece(s)], f_sem.at[w, s], dev(toward[w], e))
            if s + 1 < SPLIT:
                send_direct(s + 1)
        arrived(own_in, rs_sem.at[2])
        for s in range(SPLIT):
            at = slice(s * step_rows, (s + 1) * step_rows)
            for w in range(2):
                where = rows_of(w, s)
                for q in range(CORES):
                    arrived(dir_in.at[w, q, piece(s)], dir_sem.at[w, q, s])
                arrived(f_in.at[w, piece(s)], f_sem.at[w, s])
                v = ((part[3, e, where].astype(F32) + own_in[where].astype(F32))
                     + (dir_in[w, 0, at].astype(F32) + dir_in[w, 1, at].astype(F32)) + f_in[w, at])
                v = (x[c, e, where].astype(F32) + v).astype(BF16)
                x[c, e, where] = v
                v = v.astype(F32)
                sq = v * v
                tot = sq[:, :128]
                for j in range(1, width // 128):
                    tot = tot + sq[:, j * 128:(j + 1) * 128]
                squares[where, :] = tot
            finished(s)
        send.done()

    def reduce(chunk, consume, with_stats=True):
        send = Sends(snd2_sem)

        def push(chip, core, w, s, where):
            ref = x.at[chip, core, rows_of(w, s)]
            send(ref, ref, ag_sem.at[chip, core, w, s], where)

        def have(chip, core, w, s):
            arrived(x.at[chip, core, rows_of(w, s)], ag_sem.at[chip, core, w, s])

        def share(chip):
            ref = x.at[chip, e]
            send(ref, ref, mate_sem.at[chip], mate)

        def shared(chip):
            arrived(x.at[chip, other], mate_sem.at[chip])

        def finished(s):
            push(c, e, 0, s, dev(right, e))
            push(c, e, 1, s, dev(left, e))
            if with_stats and s == SPLIT - 1:
                row = jnp.sum(squares[...].T, axis=0, keepdims=True)
                stat[tp] = jnp.broadcast_to(row, (8, rows))
                for step in range(1, n_dev):
                    send(stat.at[tp], stat.at[tp], st_sem.at[tp], {'tp': lax.rem(tp + step, n_dev)})
            push(c, e, 1, s, dev(right, e))
            push(c, e, 0, s, dev(left, e))
            if s == SPLIT - 1:
                share(c)

        reduce_scatter(chunk, finished)
        for s in range(SPLIT):
            have(left, e, 0, s)
            push(left, e, 0, s, dev(right, e))
            have(right, e, 1, s)
            push(right, e, 1, s, dev(left, e))
        for s in range(SPLIT):
            have(left, e, 1, s)
        share(left)
        for s in range(SPLIT):
            have(right, e, 0, s)
        share(right)
        if with_stats:
            for step in range(1, n_dev):
                src = lax.rem(tp + step, n_dev)
                arrived(stat.at[src], st_sem.at[src])
            row = stat[0, 0:1]
            for j in range(1, n_dev):
                row = row + stat[j, 0:1]
            rbuf[...] = jnp.broadcast_to(lax.rsqrt(row / d_model + NORM_EPS), (rows, rows)).T
        shared(c)
        consume(0)
        shared(left)
        consume(1)
        for s in range(SPLIT):
            for w in range(2):
                have(far, e, w, s)
        share(far)
        shared(right)
        consume(2)
        consume(3, e)
        shared(far)
        consume(3, other)
        send.done()

    for i in range(chips):
        use_qkv(0)(i)
    for m in range(GU_SLOTS):
        ld_gu(m).start()
    for l in range(layers):
        attention(l)
        reduce(chunk_out(l), use_gu(l))
        gate = g_acc[...].astype(BF16).astype(F32)
        up = u_acc[...].astype(BF16).astype(F32)
        act[...] = (gate * jax.nn.sigmoid(gate) * up).astype(BF16)
        if l + 1 < layers:
            reduce(chunk_down(l), use_qkv(l + 1))
    stores = []

    def store(i, q=None):
        if q is not None and q is e:
            return
        for h in range(CORES):
            cp = pltpu.make_async_copy(
                x.at[in_order[i], h],
                out.at[:, pl.ds(pl.multiple_of(in_order[i] * wide + h * width, width), width)],
                x_sem.at[i, h])
            cp.start()
            stores.append(cp)

    reduce(chunk_down(layers - 1), store, with_stats=False)
    for cp in stores:
        cp.wait()


def emit_kernel(src, dst, buf, in_sem, out_sem):
    n = in_sem.shape[0]
    rows = src.shape[0] // n

    def copy_in(i):
        return pltpu.make_async_copy(src.at[pl.ds(i * rows, rows)], buf.at[pl.ds(i * rows, rows)], in_sem.at[i])

    def copy_out(i):
        return pltpu.make_async_copy(buf.at[pl.ds(i * rows, rows)], dst.at[pl.ds(i * rows, rows)], out_sem.at[i])

    for i in range(n):
        copy_in(i).start()
    for i in range(n):
        copy_in(i).wait()
        copy_out(i).start()
    for i in range(n):
        copy_out(i).wait()


def emit(value):
    hbm = pl.BlockSpec(memory_space=pl.ANY)
    return pl.pallas_call(
        emit_kernel, out_shape=jax.ShapeDtypeStruct(value.shape, value.dtype), in_specs=[hbm], out_specs=hbm,
        scratch_shapes=[pltpu.VMEM(value.shape, value.dtype), pltpu.SemaphoreType.DMA((8,)),
                        pltpu.SemaphoreType.DMA((8,))],
        cost_estimate=pl.CostEstimate(flops=0, bytes_accessed=4 * value.size, transcendentals=0))(value)


def solution(mesh):
    n_dev = mesh.shape['tp']
    chips = n_dev // CORES

    def local_step(hidden, lengths, k_cache, v_cache, attn_norm, w_qkv, w_out, mlp_norm, w_gate, w_up, w_down):
        layers, rows, seq, _, head_dim = k_cache.shape
        d_model = hidden.shape[1]
        width = d_model // n_dev
        qkv_cols = w_qkv.shape[3]
        group = qkv_cols // head_dim - 2
        ff = w_gate.shape[2]
        half = rows // 2
        wide = CORES * width
        heads = group * head_dim
        inv_freq = (ROPE_BASE ** (-np.arange(0, head_dim, 2, dtype=np.float32) / head_dim)).astype(np.float32)
        freq = jnp.asarray(np.concatenate([inv_freq, inv_freq])[None, :])
        cfg = (layers, rows, width, head_dim, group, chips, seq)
        vmem = pl.BlockSpec(memory_space=pltpu.VMEM)
        hbm = pl.BlockSpec(memory_space=pl.ANY)
        flops = 2 * layers * rows * d_model * (qkv_cols + heads + 3 * ff)
        return emit(pl.pallas_call(
            functools.partial(kernel, cfg),
            out_shape=jax.ShapeDtypeStruct((rows, d_model), BF16),
            in_specs=[hbm] + [vmem] * 4 + [hbm] * 7,
            out_specs=hbm,
            scratch_shapes=[
                pltpu.VMEM((chips, CORES, rows, width), BF16),
                pltpu.VMEM((rows, wide), BF16),
                pltpu.VMEM((rows, 128), F32),
                pltpu.VMEM((rows * group, seq), F32),
                pltpu.VMEM((chips, CORES, rows, width), BF16),
                pltpu.VMEM((2, CORES, half, width), BF16),
                pltpu.VMEM((2, half, width), BF16),
                pltpu.VMEM((2, CORES, half, width), BF16),
                pltpu.VMEM((rows, width), BF16),
                pltpu.VMEM((2, half, width), F32),
                pltpu.VMEM((2, half, width), F32),
                pltpu.VMEM((n_dev, 8, rows), F32),
                pltpu.VMEM((rows, 128), F32),
                pltpu.VMEM((rows, head_dim), F32),
                pltpu.VMEM((rows, head_dim), F32),
                pltpu.VMEM((rows * group, head_dim), F32),
                pltpu.VMEM((rows * group, head_dim), F32),
                pltpu.VMEM((rows * group, head_dim), F32),
                pltpu.VMEM((rows * group, seq), F32),
                pltpu.VMEM((rows, heads), BF16),
                pltpu.VMEM((rows, ff), BF16),
                pltpu.VMEM((rows, ff), F32),
                pltpu.VMEM((rows, ff), F32),
                pltpu.VMEM((rows, seq, head_dim), BF16),
                pltpu.VMEM((GU_SLOTS, wide, ff), BF16),
                pltpu.VMEM((chips, ff, wide), BF16),
                pltpu.SemaphoreType.DMA((3,)),
                pltpu.SemaphoreType.DMA((2, CORES, SPLIT)),
                pltpu.SemaphoreType.DMA((2, CORES, SPLIT)),
                pltpu.SemaphoreType.DMA((2, SPLIT)),
                pltpu.SemaphoreType.DMA((chips, CORES, 2, SPLIT)),
                pltpu.SemaphoreType.DMA((chips,)),
                pltpu.SemaphoreType.DMA((n_dev,)),
                pltpu.SemaphoreType.DMA((3 + 10 * SPLIT,)),
                pltpu.SemaphoreType.DMA((n_dev + 3 + 6 * SPLIT,)),
                pltpu.SemaphoreType.DMA((13,)),
                pltpu.SemaphoreType.DMA((16,)),
                pltpu.SemaphoreType.DMA((V_PARTS,)),
                pltpu.SemaphoreType.DMA((GU_SLOTS,)),
                pltpu.SemaphoreType.DMA((chips, CORES)),
            ],
            compiler_params=pltpu.CompilerParams(
                collective_id=0, has_side_effects=True, vmem_limit_bytes=67043328),
            cost_estimate=pl.CostEstimate(flops=flops, bytes_accessed=flops // rows, transcendentals=0),
        )(hidden, lengths.reshape(1, rows), freq, attn_norm, mlp_norm,
          w_qkv.reshape(layers, d_model, qkv_cols), w_out, w_gate, w_up, w_down,
          k_cache.reshape(layers, rows * seq, head_dim), v_cache.reshape(layers, rows, seq, head_dim)))

    cache_spec = P(None, 'dp', None, 'tp', None)
    in_specs = (P('dp', None), P('dp'), cache_spec, cache_spec, P(), P(None, None, 'tp', None),
                P(None, 'tp', None), P(), P(None, None, 'tp'), P(None, None, 'tp'), P(None, 'tp', None))
    return jax.shard_map(local_step, mesh=mesh, in_specs=in_specs, out_specs=P('dp', None), check_vma=False)
```

```python
import functools

import jax
import jax.numpy as jnp
import numpy as np
from jax import lax
from jax.experimental import pallas as pl
from jax.experimental.pallas import tpu as pltpu
from jax.sharding import PartitionSpec as P

ROPE_BASE = 10000.0
NORM_EPS = 1e-5
F32 = jnp.float32
BF16 = jnp.bfloat16
MESH = pl.DeviceIdType.MESH
CORES = 2
GU_SLOTS = 7
SPLIT = 4
V_PARTS = 2
TRIP_BLOCKS = 3
NEG = -1e30


def kernel(cfg, hid, lens, freq, gain_attn, gain_mlp, wqkv, wout, wgate, wup, wdown, kc, vc, out,
           x, a_buf, rbuf, lrep, part, rel_in, prt_in, dir_in, own_in, f_out, f_in, stat, squares, cos_ref, sin_ref,
           q_s, kn_s, vn_s, s_s, attn, act, g_acc, u_acc,
           b_v, b_gu, b_d,
           rs_sem, rel_sem, dir_sem, f_sem, ag_sem, mate_sem, st_sem, snd_sem, snd2_sem, w_sem, k_sem, v_sem, g_sem, x_sem):
    layers, rows, width, head_dim, group, chips, seq = cfg
    half = rows // 2
    wide = CORES * width
    qkv_cols = (group + 2) * head_dim
    heads = group * head_dim
    d_model = chips * wide
    tp = lax.axis_index('tp')
    e = lax.rem(tp, CORES)
    c = lax.div(tp, CORES)
    other = 1 - e
    right = lax.rem(c + 1, chips)
    left = lax.rem(c + chips - 1, chips)
    far = lax.rem(c + 2, chips)
    first = pl.ds(0, half)
    second = pl.ds(half, half)

    def dev(chip, core):
        return {'tp': chip * CORES + core}

    def cols(chip):
        return pl.ds(pl.multiple_of(chip * wide, wide), wide)

    in_order = (c, left, right, far)
    out_order = (far, right, left, c)

    def qkv_at(i):
        return b_d.at[i, 0:wide, 0:qkv_cols]

    def out_at(i):
        return b_d.at[i, wide:wide + heads, :]

    per_block = wide // seq
    lane_blocks = (wide - qkv_cols) // head_dim
    n_blocks = -(-rows // per_block)
    full_blocks = rows // per_block

    def keys_at(j, first_row, n):
        lane = pl.multiple_of(qkv_cols + (j % lane_blocks) * head_dim, head_dim)
        return b_d.at[j // lane_blocks, pl.ds(first_row, n), pl.ds(lane, head_dim)]

    def ld_qkv(l, i):
        return pltpu.make_async_copy(wqkv.at[l, cols(in_order[i]), :], qkv_at(i), w_sem.at[i])

    def ld_out(l, i):
        return pltpu.make_async_copy(wout.at[l, :, cols(out_order[i])], out_at(i), w_sem.at[4 + i])

    def ld_k(l, j):
        n = (per_block if not isinstance(j, int) or j < full_blocks else rows - j * per_block) * seq
        return pltpu.make_async_copy(kc.at[l, pl.ds(j * wide, n), :], keys_at(j, 0, n), k_sem.at[j])

    v_rows = rows // V_PARTS

    def ld_v(l, i):
        at = pl.ds(i * v_rows, v_rows)
        return pltpu.make_async_copy(vc.at[l, at], b_v.at[at], v_sem.at[i])

    def ld_gu(m):
        l, i, s = m // (2 * chips), m // 2 % chips, m % GU_SLOTS
        src = wup if m % 2 else wgate
        return pltpu.make_async_copy(src.at[l, cols(in_order[i]), :], b_gu.at[s], g_sem.at[s])

    def ld_d(l, i):
        return pltpu.make_async_copy(wdown.at[l, :, cols(out_order[i])], b_d.at[i], w_sem.at[9 + i])

    x_loads = [pltpu.make_async_copy(
        hid.at[:, pl.ds(k * wide + h * width, width)], x.at[k, h], x_sem.at[k, h])
        for k in range(chips) for h in range(CORES)]
    for cp in x_loads:
        cp.start()
    for i in range(chips):
        ld_qkv(0, i).start()
    for j in range(n_blocks):
        ld_k(0, j).start()
    for i in range(V_PARTS):
        ld_v(0, i).start()
    for i in range(chips):
        ld_out(0, i).start()

    barrier = pltpu.get_barrier_semaphore()
    n_dev = chips * CORES
    for step in range(1, n_dev):
        pl.semaphore_signal(barrier, inc=1, device_id={'tp': lax.rem(tp + step, n_dev)}, device_id_type=MESH)
    pl.semaphore_wait(barrier, n_dev - 1)

    lens_row = jnp.broadcast_to(lens[...].astype(F32), (rows, rows)).T
    for g in range(group):
        lrep[pl.ds(g, rows, stride=group), :] = lens_row
    angles = lens_row[:, :head_dim] * freq[...]
    sine = jnp.sin(angles)
    cos_ref[...] = jnp.cos(angles)
    sin_ref[...] = jnp.where(lax.broadcasted_iota(jnp.int32, angles.shape, 1) < head_dim // 2, -sine, sine)

    for cp in x_loads:
        cp.wait()
    total = jnp.zeros((rows, 128), F32)
    for k in range(chips):
        for h in range(CORES):
            for j in range(width // 128):
                v = x[k, h, :, j * 128:(j + 1) * 128].astype(F32)
                total = total + v * v
    scale0 = lax.rsqrt(jnp.sum(total, axis=1, keepdims=True) / d_model + NORM_EPS)
    rbuf[...] = jnp.broadcast_to(scale0, (rows, 128))

    def normed(chip, gain_ref, l, q):
        r = jnp.concatenate([rbuf[...]] * (width // 128), axis=1)
        at = pl.ds(pl.multiple_of(chip * wide + q * width, width), width)
        gain = gain_ref[l:l + 1, at].astype(F32)
        return (x[chip, q].astype(F32) * r * gain).astype(BF16)

    def take(i, q, gain_ref, l):
        if q is None:
            for k in range(CORES):
                a_buf[:, k * width:(k + 1) * width] = normed(in_order[i], gain_ref, l, k)
            return a_buf, pl.ds(0, wide)
        a_buf[:, 0:width] = normed(in_order[i], gain_ref, l, q)
        return a_buf.at[:, 0:width], pl.ds(pl.multiple_of(q * width, width), width)

    def use_qkv(l):
        def consume(i, q=None):
            a, at = take(i, q, gain_attn, l)
            if q is not other:
                ld_qkv(l, i).wait()
            prod = jnp.dot(a[...], qkv_at(i).at[at, :][...], preferred_element_type=F32)
            if i == 0:
                g_acc[:, :qkv_cols] = prod
            else:
                g_acc[:, :qkv_cols] += prod
        return consume

    def use_gu(l):
        def consume(i, q=None):
            a, at = take(i, q, gain_mlp, l)
            for j, acc in enumerate((g_acc, u_acc)):
                m = 2 * (l * chips + i) + j
                if q is not other:
                    ld_gu(m).wait()
                prod = jnp.dot(a[...], b_gu[m % GU_SLOTS, at, :], preferred_element_type=F32)
                if i == 0:
                    acc[...] = prod
                else:
                    acc[...] += prod
                if q is not e and m + GU_SLOTS < layers * chips * 2:
                    ld_gu(m + GU_SLOTS).start()
        return consume

    def attention(l):
        cosine, sine = cos_ref[...], sin_ref[...]

        def rot(v):
            return (v * cosine + pltpu.roll(v, head_dim // 2, 1) * sine).astype(BF16).astype(F32)

        def head(j):
            return g_acc[:, j * head_dim:(j + 1) * head_dim].astype(BF16).astype(F32)

        key_new = rot(head(group))
        val_new = head(group + 1)
        for g in range(group):
            at = pl.ds(g, rows, stride=group)
            q_s[at, :] = rot(head(g))
            kn_s[at, :] = key_new
            vn_s[at, :] = val_new
        scale = head_dim ** -0.5
        pair = 2 * group
        upper = lax.broadcasted_iota(jnp.int32, (pair, head_dim), 0) < group
        def score(j, p):
            at = pl.ds(pl.multiple_of((j * (per_block // 2) + p) * pair, pair), pair)
            keys = keys_at(j, p * 2 * seq, 2 * seq)[...]
            s = lax.dot_general(q_s[at, :].astype(BF16), keys, (((1,), (1,)), ((), ())),
                                preferred_element_type=F32)
            s_s[at, :] = jnp.where(upper, s[:, :seq], s[:, seq:])

        def scores(n, carry):
            for k in range(TRIP_BLOCKS):
                ld_k(l, n * TRIP_BLOCKS + k).wait()
            for k in range(TRIP_BLOCKS):
                for p in range(per_block // 2):
                    score(n * TRIP_BLOCKS + k, p)
            return carry

        lax.fori_loop(0, full_blocks // TRIP_BLOCKS, scores, 0)
        for j in range(full_blocks // TRIP_BLOCKS * TRIP_BLOCKS, full_blocks):
            ld_k(l, j).wait()
            for p in range(per_block // 2):
                score(j, p)
        if full_blocks < n_blocks:
            ld_k(l, full_blocks).wait()
        for p in range((rows - full_blocks * per_block) // 2):
            score(full_blocks, p)
        pos = lax.broadcasted_iota(jnp.int32, (rows * group, seq), 1).astype(F32)
        s = jnp.where(pos < lrep[...], s_s[...] * scale, NEG)
        own = jnp.sum(q_s[...] * kn_s[...], axis=1, keepdims=True) * scale
        peak = jnp.maximum(jnp.max(s, axis=1, keepdims=True), own)
        w = jnp.exp(s - peak).astype(BF16).astype(F32)
        w_own = jnp.exp(own - peak).astype(BF16).astype(F32)
        denom = jnp.sum(w, axis=1, keepdims=True) + w_own
        s_s[...] = w
        q_s[...] = w_own * vn_s[...]
        kn_s[...] = jnp.broadcast_to(denom, kn_s.shape)

        def mix(i, carry):
            ld_v(l, i).wait()
            for p in range(v_rows // 2):
                n = i * (v_rows // 2) + p
                at = pl.ds(pl.multiple_of(n * pair, pair), pair)
                w = s_s[at, :].astype(BF16)
                vals = jnp.concatenate([b_v[n * 2], b_v[n * 2 + 1]], axis=1)
                o = jnp.dot(w, vals, preferred_element_type=F32)
                o = jnp.where(upper, o[:, :head_dim], o[:, head_dim:])
                s_s[at, :] = (o + q_s[at, :]) / kn_s[at, :]
            return carry

        lax.fori_loop(0, V_PARTS, mix, 0)
        if l + 1 < layers:
            for i in range(V_PARTS):
                ld_v(l + 1, i).start()
        for g in range(group):
            attn[:, g * head_dim:(g + 1) * head_dim] = s_s[pl.ds(g, rows, stride=group), :].astype(BF16)

    def multiply(a, w, i, sent):
        if sent is None:
            prod = jnp.dot(a[...], w[...], preferred_element_type=F32)
            part[i, 0] = prod[:, :width].astype(BF16)
            part[i, 1] = prod[:, width:].astype(BF16)
            return
        for q in range(CORES):
            part[i, q] = jnp.dot(a[...], w[:, q * width:(q + 1) * width], preferred_element_type=F32).astype(BF16)
            sent(q)

    def chunk_out(l):
        def chunk(i, sent=None):
            ld_out(l, i).wait()
            multiply(attn, out_at(i), i, sent)
            ld_d(l, i).start()
        return chunk

    def chunk_down(l):
        def chunk(i, sent=None):
            ld_d(l, i).wait()
            multiply(act, b_d.at[i], i, sent)
            if l + 1 < layers:
                ld_qkv(l + 1, i).start()
                for j in range(n_blocks):
                    if j // lane_blocks == i:
                        ld_k(l + 1, j).start()
                if i == chips - 1:
                    for k in range(chips):
                        ld_out(l + 1, k).start()
        return chunk

    step_rows = half // SPLIT

    def rows_of(w, s):
        return pl.ds(w * half + s * step_rows, step_rows)

    def remote(src, dst, ssem, rsem, where):
        return pltpu.make_async_remote_copy(
            src_ref=src, dst_ref=dst, send_sem=ssem, recv_sem=rsem, device_id=where, device_id_type=MESH)

    me = dev(c, e)
    mate = dev(c, other)

    def arrived(dst, rsem):
        remote(dst, dst, rsem, rsem, me).wait_recv()

    class Sends:
        def __init__(self, sems):
            self.sems, self.all = sems, []

        def __call__(self, src, dst, rsem, where):
            cp = remote(src, dst, self.sems.at[len(self.all)], rsem, where)
            cp.start()
            self.all.append(cp)

        def done(self):
            for cp in self.all:
                cp.wait_send()

    toward = (right, left)

    def reduce_scatter(chunk, finished):
        send = Sends(snd_sem)

        def piece(s):
            return pl.ds(s * step_rows, step_rows)

        def send_direct(s):
            for q in range(CORES):
                send(part.at[1, q, rows_of(1, s)], dir_in.at[1, e, piece(s)], dir_sem.at[1, e, s], dev(right, q))
                send(part.at[2, q, rows_of(0, s)], dir_in.at[0, e, piece(s)], dir_sem.at[0, e, s], dev(left, q))

        def send_far(q):
            for s in range(SPLIT):
                for w in range(2):
                    send(part.at[0, q, rows_of(w, s)], rel_in.at[w, e, piece(s)], rel_sem.at[w, e, s],
                         dev(toward[w], q))

        chunk(0, send_far)
        chunk(1)
        send(part.at[1, other, first], prt_in.at[0], rs_sem.at[0], mate)
        chunk(2)
        send(part.at[2, other, second], prt_in.at[1], rs_sem.at[1], mate)
        send_direct(0)
        chunk(3)
        send(part.at[3, other], own_in, rs_sem.at[2], mate)
        for w in range(2):
            arrived(prt_in.at[w], rs_sem.at[w])
        for s in range(SPLIT):
            at = slice(s * step_rows, (s + 1) * step_rows)
            for w in range(2):
                for q in range(CORES):
                    arrived(rel_in.at[w, q, piece(s)], rel_sem.at[w, q, s])
                f_out[w, at] = (rel_in[w, 0, at].astype(F32) + rel_in[w, 1, at].astype(F32)
                                + (prt_in[w, at].astype(F32) + part[1 + w, e, rows_of(w, s)].astype(F32)))
                send(f_out.at[w, piece(s)], f_in.at[w, piece(s)], f_sem.at[w, s], dev(toward[w], e))
            if s + 1 < SPLIT:
                send_direct(s + 1)
        arrived(own_in, rs_sem.at[2])
        for s in range(SPLIT):
            at = slice(s * step_rows, (s + 1) * step_rows)
            for w in range(2):
                where = rows_of(w, s)
                for q in range(CORES):
                    arrived(dir_in.at[w, q, piece(s)], dir_sem.at[w, q, s])
                arrived(f_in.at[w, piece(s)], f_sem.at[w, s])
                v = ((part[3, e, where].astype(F32) + own_in[where].astype(F32))
                     + (dir_in[w, 0, at].astype(F32) + dir_in[w, 1, at].astype(F32)) + f_in[w, at])
                v = (x[c, e, where].astype(F32) + v).astype(BF16)
                x[c, e, where] = v
                v = v.astype(F32)
                sq = v * v
                tot = sq[:, :128]
                for j in range(1, width // 128):
                    tot = tot + sq[:, j * 128:(j + 1) * 128]
                squares[where, :] = tot
            finished(s)
        send.done()

    def reduce(chunk, consume, with_stats=True):
        send = Sends(snd2_sem)

        def push(chip, core, w, s, where):
            ref = x.at[chip, core, rows_of(w, s)]
            send(ref, ref, ag_sem.at[chip, core, w, s], where)

        def have(chip, core, w, s):
            arrived(x.at[chip, core, rows_of(w, s)], ag_sem.at[chip, core, w, s])

        def share(chip):
            ref = x.at[chip, e]
            send(ref, ref, mate_sem.at[chip], mate)

        def shared(chip):
            arrived(x.at[chip, other], mate_sem.at[chip])

        def finished(s):
            push(c, e, 0, s, dev(right, e))
            push(c, e, 1, s, dev(left, e))
            if with_stats and s == SPLIT - 1:
                row = jnp.sum(squares[...].T, axis=0, keepdims=True)
                stat[tp] = jnp.broadcast_to(row, (8, rows))
                for step in range(1, n_dev):
                    send(stat.at[tp], stat.at[tp], st_sem.at[tp], {'tp': lax.rem(tp + step, n_dev)})
            push(c, e, 1, s, dev(right, e))
            push(c, e, 0, s, dev(left, e))
            if s == SPLIT - 1:
                share(c)

        reduce_scatter(chunk, finished)
        for s in range(SPLIT):
            have(left, e, 0, s)
            push(left, e, 0, s, dev(right, e))
            have(right, e, 1, s)
            push(right, e, 1, s, dev(left, e))
        for s in range(SPLIT):
            have(left, e, 1, s)
        share(left)
        for s in range(SPLIT):
            have(right, e, 0, s)
        share(right)
        if with_stats:
            for step in range(1, n_dev):
                src = lax.rem(tp + step, n_dev)
                arrived(stat.at[src], st_sem.at[src])
            row = stat[0, 0:1]
            for j in range(1, n_dev):
                row = row + stat[j, 0:1]
            rbuf[...] = jnp.broadcast_to(lax.rsqrt(row / d_model + NORM_EPS), (rows, rows)).T
        shared(c)
        consume(0)
        shared(left)
        consume(1)
        shared(right)
        consume(2)
        for s in range(SPLIT):
            for w in range(2):
                have(far, e, w, s)
        share(far)
        consume(3, e)
        shared(far)
        consume(3, other)
        send.done()

    for i in range(chips):
        use_qkv(0)(i)
    for m in range(GU_SLOTS):
        ld_gu(m).start()
    for l in range(layers):
        attention(l)
        reduce(chunk_out(l), use_gu(l))
        gate = g_acc[...].astype(BF16).astype(F32)
        up = u_acc[...].astype(BF16).astype(F32)
        act[...] = (gate * jax.nn.sigmoid(gate) * up).astype(BF16)
        if l + 1 < layers:
            reduce(chunk_down(l), use_qkv(l + 1))
    stores = []

    def store(i, q=None):
        if q is not None and q is e:
            return
        for h in range(CORES):
            cp = pltpu.make_async_copy(
                x.at[in_order[i], h],
                out.at[:, pl.ds(pl.multiple_of(in_order[i] * wide + h * width, width), width)],
                x_sem.at[i, h])
            cp.start()
            stores.append(cp)

    reduce(chunk_down(layers - 1), store, with_stats=False)
    for cp in stores:
        cp.wait()


def emit_kernel(src, dst, buf, in_sem, out_sem):
    n = in_sem.shape[0]
    rows = src.shape[0] // n

    def copy_in(i):
        return pltpu.make_async_copy(src.at[pl.ds(i * rows, rows)], buf.at[pl.ds(i * rows, rows)], in_sem.at[i])

    def copy_out(i):
        return pltpu.make_async_copy(buf.at[pl.ds(i * rows, rows)], dst.at[pl.ds(i * rows, rows)], out_sem.at[i])

    for i in range(n):
        copy_in(i).start()
    for i in range(n):
        copy_in(i).wait()
        copy_out(i).start()
    for i in range(n):
        copy_out(i).wait()


def emit(value):
    hbm = pl.BlockSpec(memory_space=pl.ANY)
    return pl.pallas_call(
        emit_kernel, out_shape=jax.ShapeDtypeStruct(value.shape, value.dtype), in_specs=[hbm], out_specs=hbm,
        scratch_shapes=[pltpu.VMEM(value.shape, value.dtype), pltpu.SemaphoreType.DMA((8,)),
                        pltpu.SemaphoreType.DMA((8,))],
        cost_estimate=pl.CostEstimate(flops=0, bytes_accessed=4 * value.size, transcendentals=0))(value)


def solution(mesh):
    n_dev = mesh.shape['tp']
    chips = n_dev // CORES

    def local_step(hidden, lengths, k_cache, v_cache, attn_norm, w_qkv, w_out, mlp_norm, w_gate, w_up, w_down):
        layers, rows, seq, _, head_dim = k_cache.shape
        d_model = hidden.shape[1]
        width = d_model // n_dev
        qkv_cols = w_qkv.shape[3]
        group = qkv_cols // head_dim - 2
        ff = w_gate.shape[2]
        half = rows // 2
        wide = CORES * width
        heads = group * head_dim
        inv_freq = (ROPE_BASE ** (-np.arange(0, head_dim, 2, dtype=np.float32) / head_dim)).astype(np.float32)
        freq = jnp.asarray(np.concatenate([inv_freq, inv_freq])[None, :])
        cfg = (layers, rows, width, head_dim, group, chips, seq)
        vmem = pl.BlockSpec(memory_space=pltpu.VMEM)
        hbm = pl.BlockSpec(memory_space=pl.ANY)
        flops = 2 * layers * rows * d_model * (qkv_cols + heads + 3 * ff)
        return emit(pl.pallas_call(
            functools.partial(kernel, cfg),
            out_shape=jax.ShapeDtypeStruct((rows, d_model), BF16),
            in_specs=[hbm] + [vmem] * 4 + [hbm] * 7,
            out_specs=hbm,
            scratch_shapes=[
                pltpu.VMEM((chips, CORES, rows, width), BF16),
                pltpu.VMEM((rows, wide), BF16),
                pltpu.VMEM((rows, 128), F32),
                pltpu.VMEM((rows * group, seq), F32),
                pltpu.VMEM((chips, CORES, rows, width), BF16),
                pltpu.VMEM((2, CORES, half, width), BF16),
                pltpu.VMEM((2, half, width), BF16),
                pltpu.VMEM((2, CORES, half, width), BF16),
                pltpu.VMEM((rows, width), BF16),
                pltpu.VMEM((2, half, width), F32),
                pltpu.VMEM((2, half, width), F32),
                pltpu.VMEM((n_dev, 8, rows), F32),
                pltpu.VMEM((rows, 128), F32),
                pltpu.VMEM((rows, head_dim), F32),
                pltpu.VMEM((rows, head_dim), F32),
                pltpu.VMEM((rows * group, head_dim), F32),
                pltpu.VMEM((rows * group, head_dim), F32),
                pltpu.VMEM((rows * group, head_dim), F32),
                pltpu.VMEM((rows * group, seq), F32),
                pltpu.VMEM((rows, heads), BF16),
                pltpu.VMEM((rows, ff), BF16),
                pltpu.VMEM((rows, ff), F32),
                pltpu.VMEM((rows, ff), F32),
                pltpu.VMEM((rows, seq, head_dim), BF16),
                pltpu.VMEM((GU_SLOTS, wide, ff), BF16),
                pltpu.VMEM((chips, ff, wide), BF16),
                pltpu.SemaphoreType.DMA((3,)),
                pltpu.SemaphoreType.DMA((2, CORES, SPLIT)),
                pltpu.SemaphoreType.DMA((2, CORES, SPLIT)),
                pltpu.SemaphoreType.DMA((2, SPLIT)),
                pltpu.SemaphoreType.DMA((chips, CORES, 2, SPLIT)),
                pltpu.SemaphoreType.DMA((chips,)),
                pltpu.SemaphoreType.DMA((n_dev,)),
                pltpu.SemaphoreType.DMA((3 + 10 * SPLIT,)),
                pltpu.SemaphoreType.DMA((n_dev + 3 + 6 * SPLIT,)),
                pltpu.SemaphoreType.DMA((13,)),
                pltpu.SemaphoreType.DMA((16,)),
                pltpu.SemaphoreType.DMA((V_PARTS,)),
                pltpu.SemaphoreType.DMA((GU_SLOTS,)),
                pltpu.SemaphoreType.DMA((chips, CORES)),
            ],
            compiler_params=pltpu.CompilerParams(
                collective_id=0, has_side_effects=True, vmem_limit_bytes=67043328),
            cost_estimate=pl.CostEstimate(flops=flops, bytes_accessed=flops // rows, transcendentals=0),
        )(hidden, lengths.reshape(1, rows), freq, attn_norm, mlp_norm,
          w_qkv.reshape(layers, d_model, qkv_cols), w_out, w_gate, w_up, w_down,
          k_cache.reshape(layers, rows * seq, head_dim), v_cache.reshape(layers, rows, seq, head_dim)))

    cache_spec = P(None, 'dp', None, 'tp', None)
    in_specs = (P('dp', None), P('dp'), cache_spec, cache_spec, P(), P(None, None, 'tp', None),
                P(None, 'tp', None), P(), P(None, None, 'tp'), P(None, None, 'tp'), P(None, 'tp', None))
    return jax.shard_map(local_step, mesh=mesh, in_specs=in_specs, out_specs=P('dp', None), check_vma=False)
```

```python
import functools

import jax
import jax.numpy as jnp
import numpy as np
from jax import lax
from jax.experimental import pallas as pl
from jax.experimental.pallas import tpu as pltpu
from jax.sharding import PartitionSpec as P

ROPE_BASE = 10000.0
NORM_EPS = 1e-5
F32 = jnp.float32
BF16 = jnp.bfloat16
MESH = pl.DeviceIdType.MESH
CORES = 2
GU_SLOTS = 7
SPLIT = 4
V_PARTS = 2
TRIP_BLOCKS = 3
NEG = -1e30


def kernel(cfg, hid, lens, freq, gain_attn, gain_mlp, wqkv, wout, wgate, wup, wdown, kc, vc, out,
           x, a_buf, rbuf, lrep, part, rel_in, prt_in, dir_in, own_in, f_out, f_in, stat, squares, cos_ref, sin_ref,
           q_s, kn_s, vn_s, s_s, attn, act, g_acc, u_acc,
           b_v, b_gu, b_d,
           rs_sem, rel_sem, dir_sem, f_sem, ag_sem, mate_sem, st_sem, snd_sem, snd2_sem, w_sem, k_sem, v_sem, g_sem, x_sem):
    layers, rows, width, head_dim, group, chips, seq = cfg
    half = rows // 2
    wide = CORES * width
    qkv_cols = (group + 2) * head_dim
    heads = group * head_dim
    d_model = chips * wide
    tp = lax.axis_index('tp')
    e = lax.rem(tp, CORES)
    c = lax.div(tp, CORES)
    other = 1 - e
    right = lax.rem(c + 1, chips)
    left = lax.rem(c + chips - 1, chips)
    far = lax.rem(c + 2, chips)
    first = pl.ds(0, half)
    second = pl.ds(half, half)

    def dev(chip, core):
        return {'tp': chip * CORES + core}

    def cols(chip):
        return pl.ds(pl.multiple_of(chip * wide, wide), wide)

    in_order = (c, left, right, far)
    out_order = (far, right, left, c)

    def qkv_at(i):
        return b_d.at[i, 0:wide, 0:qkv_cols]

    def out_at(i):
        return b_d.at[i, wide:wide + heads, :]

    per_block = wide // seq
    lane_blocks = (wide - qkv_cols) // head_dim
    n_blocks = -(-rows // per_block)
    full_blocks = rows // per_block

    def keys_at(j, first_row, n):
        lane = pl.multiple_of(qkv_cols + (j % lane_blocks) * head_dim, head_dim)
        return b_d.at[j // lane_blocks, pl.ds(first_row, n), pl.ds(lane, head_dim)]

    def ld_qkv(l, i):
        return pltpu.make_async_copy(wqkv.at[l, cols(in_order[i]), :], qkv_at(i), w_sem.at[i])

    def ld_out(l, i):
        return pltpu.make_async_copy(wout.at[l, :, cols(out_order[i])], out_at(i), w_sem.at[4 + i])

    def ld_k(l, j):
        n = (per_block if not isinstance(j, int) or j < full_blocks else rows - j * per_block) * seq
        return pltpu.make_async_copy(kc.at[l, pl.ds(j * wide, n), :], keys_at(j, 0, n), k_sem.at[j])

    v_rows = rows // V_PARTS

    def ld_v(l, i):
        at = pl.ds(i * v_rows, v_rows)
        return pltpu.make_async_copy(vc.at[l, at], b_v.at[at], v_sem.at[i])

    def ld_gu(m):
        l, i, s = m // (2 * chips), m // 2 % chips, m % GU_SLOTS
        src = wup if m % 2 else wgate
        return pltpu.make_async_copy(src.at[l, cols(in_order[i]), :], b_gu.at[s], g_sem.at[s])

    def ld_d(l, i):
        return pltpu.make_async_copy(wdown.at[l, :, cols(out_order[i])], b_d.at[i], w_sem.at[9 + i])

    x_loads = [pltpu.make_async_copy(
        hid.at[:, pl.ds(k * wide + h * width, width)], x.at[k, h], x_sem.at[k, h])
        for k in range(chips) for h in range(CORES)]
    for cp in x_loads:
        cp.start()
    for i in range(chips):
        ld_qkv(0, i).start()
    for j in range(n_blocks):
        ld_k(0, j).start()
    for i in range(V_PARTS):
        ld_v(0, i).start()
    for i in range(chips):
        ld_out(0, i).start()

    barrier = pltpu.get_barrier_semaphore()
    n_dev = chips * CORES
    for step in range(1, n_dev):
        pl.semaphore_signal(barrier, inc=1, device_id={'tp': lax.rem(tp + step, n_dev)}, device_id_type=MESH)
    pl.semaphore_wait(barrier, n_dev - 1)

    lens_row = jnp.broadcast_to(lens[...].astype(F32), (rows, rows)).T
    for g in range(group):
        lrep[pl.ds(g, rows, stride=group), :] = lens_row
    angles = lens_row[:, :head_dim] * freq[...]
    sine = jnp.sin(angles)
    cos_ref[...] = jnp.cos(angles)
    sin_ref[...] = jnp.where(lax.broadcasted_iota(jnp.int32, angles.shape, 1) < head_dim // 2, -sine, sine)

    for cp in x_loads:
        cp.wait()
    total = jnp.zeros((rows, 128), F32)
    for k in range(chips):
        for h in range(CORES):
            for j in range(width // 128):
                v = x[k, h, :, j * 128:(j + 1) * 128].astype(F32)
                total = total + v * v
    scale0 = lax.rsqrt(jnp.sum(total, axis=1, keepdims=True) / d_model + NORM_EPS)
    rbuf[...] = jnp.broadcast_to(scale0, (rows, 128))

    def normed(chip, gain_ref, l, q):
        r = jnp.concatenate([rbuf[...]] * (width // 128), axis=1)
        at = pl.ds(pl.multiple_of(chip * wide + q * width, width), width)
        gain = gain_ref[l:l + 1, at].astype(F32)
        return (x[chip, q].astype(F32) * r * gain).astype(BF16)

    def take(i, q, gain_ref, l):
        if q is None:
            for k in range(CORES):
                a_buf[:, k * width:(k + 1) * width] = normed(in_order[i], gain_ref, l, k)
            return a_buf, pl.ds(0, wide)
        a_buf[:, 0:width] = normed(in_order[i], gain_ref, l, q)
        return a_buf.at[:, 0:width], pl.ds(pl.multiple_of(q * width, width), width)

    def use_qkv(l):
        def consume(i, q=None):
            a, at = take(i, q, gain_attn, l)
            if q is not other:
                ld_qkv(l, i).wait()
            prod = jnp.dot(a[...], qkv_at(i).at[at, :][...], preferred_element_type=F32)
            if i == 0:
                g_acc[:, :qkv_cols] = prod
            else:
                g_acc[:, :qkv_cols] += prod
        return consume

    def use_gu(l):
        def consume(i, q=None):
            a, at = take(i, q, gain_mlp, l)
            for j, acc in enumerate((g_acc, u_acc)):
                m = 2 * (l * chips + i) + j
                if q is not other:
                    ld_gu(m).wait()
                prod = jnp.dot(a[...], b_gu[m % GU_SLOTS, at, :], preferred_element_type=F32)
                if i == 0:
                    acc[...] = prod
                else:
                    acc[...] += prod
                if q is not e and m + GU_SLOTS < layers * chips * 2:
                    ld_gu(m + GU_SLOTS).start()
        return consume

    def attention(l):
        cosine, sine = cos_ref[...], sin_ref[...]

        def rot(v):
            return (v * cosine + pltpu.roll(v, head_dim // 2, 1) * sine).astype(BF16).astype(F32)

        def head(j):
            return g_acc[:, j * head_dim:(j + 1) * head_dim].astype(BF16).astype(F32)

        key_new = rot(head(group))
        val_new = head(group + 1)
        for g in range(group):
            at = pl.ds(g, rows, stride=group)
            q_s[at, :] = rot(head(g))
            kn_s[at, :] = key_new
            vn_s[at, :] = val_new
        scale = head_dim ** -0.5
        pair = 2 * group
        upper = lax.broadcasted_iota(jnp.int32, (pair, head_dim), 0) < group
        def score(j, p):
            at = pl.ds(pl.multiple_of((j * (per_block // 2) + p) * pair, pair), pair)
            keys = keys_at(j, p * 2 * seq, 2 * seq)[...]
            s = lax.dot_general(q_s[at, :].astype(BF16), keys, (((1,), (1,)), ((), ())),
                                preferred_element_type=F32)
            s_s[at, :] = jnp.where(upper, s[:, :seq], s[:, seq:])

        def scores(n, carry):
            for k in range(TRIP_BLOCKS):
                ld_k(l, n * TRIP_BLOCKS + k).wait()
            for k in range(TRIP_BLOCKS):
                for p in range(per_block // 2):
                    score(n * TRIP_BLOCKS + k, p)
            return carry

        lax.fori_loop(0, full_blocks // TRIP_BLOCKS, scores, 0)
        for j in range(full_blocks // TRIP_BLOCKS * TRIP_BLOCKS, full_blocks):
            ld_k(l, j).wait()
            for p in range(per_block // 2):
                score(j, p)
        if full_blocks < n_blocks:
            ld_k(l, full_blocks).wait()
        for p in range((rows - full_blocks * per_block) // 2):
            score(full_blocks, p)
        pos = lax.broadcasted_iota(jnp.int32, (rows * group, seq), 1).astype(F32)
        s = jnp.where(pos < lrep[...], s_s[...] * scale, NEG)
        own = jnp.sum(q_s[...] * kn_s[...], axis=1, keepdims=True) * scale
        peak = jnp.maximum(jnp.max(s, axis=1, keepdims=True), own)
        w = jnp.exp(s - peak).astype(BF16).astype(F32)
        w_own = jnp.exp(own - peak).astype(BF16).astype(F32)
        denom = jnp.sum(w, axis=1, keepdims=True) + w_own
        s_s[...] = w
        q_s[...] = w_own * vn_s[...]
        kn_s[...] = jnp.broadcast_to(denom, kn_s.shape)

        def mix(i, carry):
            ld_v(l, i).wait()
            for p in range(v_rows // 2):
                n = i * (v_rows // 2) + p
                at = pl.ds(pl.multiple_of(n * pair, pair), pair)
                w = s_s[at, :].astype(BF16)
                vals = jnp.concatenate([b_v[n * 2], b_v[n * 2 + 1]], axis=1)
                o = jnp.dot(w, vals, preferred_element_type=F32)
                o = jnp.where(upper, o[:, :head_dim], o[:, head_dim:])
                s_s[at, :] = (o + q_s[at, :]) / kn_s[at, :]
            return carry

        lax.fori_loop(0, V_PARTS, mix, 0)
        if l + 1 < layers:
            for i in range(V_PARTS):
                ld_v(l + 1, i).start()
        for g in range(group):
            attn[:, g * head_dim:(g + 1) * head_dim] = s_s[pl.ds(g, rows, stride=group), :].astype(BF16)

    def multiply(a, w, i, sent):
        if sent is None:
            prod = jnp.dot(a[...], w[...], preferred_element_type=F32)
            part[i, 0] = prod[:, :width].astype(BF16)
            part[i, 1] = prod[:, width:].astype(BF16)
            return
        for q in range(CORES):
            part[i, q] = jnp.dot(a[...], w[:, q * width:(q + 1) * width], preferred_element_type=F32).astype(BF16)
            sent(q)

    def chunk_out(l):
        def chunk(i, sent=None):
            ld_out(l, i).wait()
            multiply(attn, out_at(i), i, sent)
            ld_d(l, i).start()
        return chunk

    def chunk_down(l):
        def chunk(i, sent=None):
            ld_d(l, i).wait()
            multiply(act, b_d.at[i], i, sent)
            if l + 1 < layers:
                ld_qkv(l + 1, i).start()
                for j in range(n_blocks):
                    if j // lane_blocks == i:
                        ld_k(l + 1, j).start()
                if i == chips - 1:
                    for k in range(chips):
                        ld_out(l + 1, k).start()
        return chunk

    step_rows = half // SPLIT

    def rows_of(w, s):
        return pl.ds(w * half + s * step_rows, step_rows)

    def remote(src, dst, ssem, rsem, where):
        return pltpu.make_async_remote_copy(
            src_ref=src, dst_ref=dst, send_sem=ssem, recv_sem=rsem, device_id=where, device_id_type=MESH)

    me = dev(c, e)
    mate = dev(c, other)

    def arrived(dst, rsem):
        remote(dst, dst, rsem, rsem, me).wait_recv()

    class Sends:
        def __init__(self, sems):
            self.sems, self.all = sems, []

        def __call__(self, src, dst, rsem, where):
            cp = remote(src, dst, self.sems.at[len(self.all)], rsem, where)
            cp.start()
            self.all.append(cp)

        def done(self):
            for cp in self.all:
                cp.wait_send()

    toward = (right, left)

    def reduce_scatter(chunk, finished):
        send = Sends(snd_sem)

        def piece(s):
            return pl.ds(s * step_rows, step_rows)

        def send_direct(q):
            for s in range(SPLIT):
                send(part.at[1, q, rows_of(1, s)], dir_in.at[1, e, piece(s)], dir_sem.at[1, e, s], dev(right, q))
                send(part.at[2, q, rows_of(0, s)], dir_in.at[0, e, piece(s)], dir_sem.at[0, e, s], dev(left, q))

        def send_far(q):
            for s in range(SPLIT):
                for w in range(2):
                    send(part.at[0, q, rows_of(w, s)], rel_in.at[w, e, piece(s)], rel_sem.at[w, e, s],
                         dev(toward[w], q))

        chunk(0, send_far)
        chunk(1)
        send(part.at[1, other, first], prt_in.at[0], rs_sem.at[0], mate)
        chunk(2)
        send(part.at[2, other, second], prt_in.at[1], rs_sem.at[1], mate)
        send_direct(0)
        chunk(3)
        send(part.at[3, other], own_in, rs_sem.at[2], mate)
        for w in range(2):
            arrived(prt_in.at[w], rs_sem.at[w])
        for s in range(SPLIT):
            at = slice(s * step_rows, (s + 1) * step_rows)
            for w in range(2):
                for q in range(CORES):
                    arrived(rel_in.at[w, q, piece(s)], rel_sem.at[w, q, s])
                f_out[w, at] = (rel_in[w, 0, at].astype(F32) + rel_in[w, 1, at].astype(F32)
                                + (prt_in[w, at].astype(F32) + part[1 + w, e, rows_of(w, s)].astype(F32)))
                send(f_out.at[w, piece(s)], f_in.at[w, piece(s)], f_sem.at[w, s], dev(toward[w], e))
        send_direct(1)
        arrived(own_in, rs_sem.at[2])
        for s in range(SPLIT):
            at = slice(s * step_rows, (s + 1) * step_rows)
            for w in range(2):
                where = rows_of(w, s)
                for q in range(CORES):
                    arrived(dir_in.at[w, q, piece(s)], dir_sem.at[w, q, s])
                arrived(f_in.at[w, piece(s)], f_sem.at[w, s])
                v = ((part[3, e, where].astype(F32) + own_in[where].astype(F32))
                     + (dir_in[w, 0, at].astype(F32) + dir_in[w, 1, at].astype(F32)) + f_in[w, at])
                v = (x[c, e, where].astype(F32) + v).astype(BF16)
                x[c, e, where] = v
                v = v.astype(F32)
                sq = v * v
                tot = sq[:, :128]
                for j in range(1, width // 128):
                    tot = tot + sq[:, j * 128:(j + 1) * 128]
                squares[where, :] = tot
            finished(s)
        send.done()

    def reduce(chunk, consume, with_stats=True):
        send = Sends(snd2_sem)

        def push(chip, core, w, s, where):
            ref = x.at[chip, core, rows_of(w, s)]
            send(ref, ref, ag_sem.at[chip, core, w, s], where)

        def have(chip, core, w, s):
            arrived(x.at[chip, core, rows_of(w, s)], ag_sem.at[chip, core, w, s])

        def share(chip):
            ref = x.at[chip, e]
            send(ref, ref, mate_sem.at[chip], mate)

        def shared(chip):
            arrived(x.at[chip, other], mate_sem.at[chip])

        def finished(s):
            push(c, e, 0, s, dev(right, e))
            push(c, e, 1, s, dev(left, e))
            if with_stats and s == SPLIT - 1:
                row = jnp.sum(squares[...].T, axis=0, keepdims=True)
                stat[tp] = jnp.broadcast_to(row, (8, rows))
                for step in range(1, n_dev):
                    send(stat.at[tp], stat.at[tp], st_sem.at[tp], {'tp': lax.rem(tp + step, n_dev)})
            push(c, e, 1, s, dev(right, e))
            push(c, e, 0, s, dev(left, e))
            if s == SPLIT - 1:
                share(c)

        reduce_scatter(chunk, finished)
        for s in range(SPLIT):
            have(left, e, 0, s)
            push(left, e, 0, s, dev(right, e))
            have(right, e, 1, s)
            push(right, e, 1, s, dev(left, e))
        for s in range(SPLIT):
            have(left, e, 1, s)
        share(left)
        for s in range(SPLIT):
            have(right, e, 0, s)
        share(right)
        if with_stats:
            for step in range(1, n_dev):
                src = lax.rem(tp + step, n_dev)
                arrived(stat.at[src], st_sem.at[src])
            row = stat[0, 0:1]
            for j in range(1, n_dev):
                row = row + stat[j, 0:1]
            rbuf[...] = jnp.broadcast_to(lax.rsqrt(row / d_model + NORM_EPS), (rows, rows)).T
        shared(c)
        consume(0)
        shared(left)
        consume(1)
        shared(right)
        consume(2)
        for s in range(SPLIT):
            for w in range(2):
                have(far, e, w, s)
        share(far)
        consume(3, e)
        shared(far)
        consume(3, other)
        send.done()

    for i in range(chips):
        use_qkv(0)(i)
    for m in range(GU_SLOTS):
        ld_gu(m).start()
    for l in range(layers):
        attention(l)
        reduce(chunk_out(l), use_gu(l))
        gate = g_acc[...].astype(BF16).astype(F32)
        up = u_acc[...].astype(BF16).astype(F32)
        act[...] = (gate * jax.nn.sigmoid(gate) * up).astype(BF16)
        if l + 1 < layers:
            reduce(chunk_down(l), use_qkv(l + 1))
    stores = []

    def store(i, q=None):
        if q is not None and q is e:
            return
        for h in range(CORES):
            cp = pltpu.make_async_copy(
                x.at[in_order[i], h],
                out.at[:, pl.ds(pl.multiple_of(in_order[i] * wide + h * width, width), width)],
                x_sem.at[i, h])
            cp.start()
            stores.append(cp)

    reduce(chunk_down(layers - 1), store, with_stats=False)
    for cp in stores:
        cp.wait()


def emit_kernel(src, dst, buf, in_sem, out_sem):
    n = in_sem.shape[0]
    rows = src.shape[0] // n

    def copy_in(i):
        return pltpu.make_async_copy(src.at[pl.ds(i * rows, rows)], buf.at[pl.ds(i * rows, rows)], in_sem.at[i])

    def copy_out(i):
        return pltpu.make_async_copy(buf.at[pl.ds(i * rows, rows)], dst.at[pl.ds(i * rows, rows)], out_sem.at[i])

    for i in range(n):
        copy_in(i).start()
    for i in range(n):
        copy_in(i).wait()
        copy_out(i).start()
    for i in range(n):
        copy_out(i).wait()


def emit(value):
    hbm = pl.BlockSpec(memory_space=pl.ANY)
    return pl.pallas_call(
        emit_kernel, out_shape=jax.ShapeDtypeStruct(value.shape, value.dtype), in_specs=[hbm], out_specs=hbm,
        scratch_shapes=[pltpu.VMEM(value.shape, value.dtype), pltpu.SemaphoreType.DMA((8,)),
                        pltpu.SemaphoreType.DMA((8,))],
        cost_estimate=pl.CostEstimate(flops=0, bytes_accessed=4 * value.size, transcendentals=0))(value)


def solution(mesh):
    n_dev = mesh.shape['tp']
    chips = n_dev // CORES

    def local_step(hidden, lengths, k_cache, v_cache, attn_norm, w_qkv, w_out, mlp_norm, w_gate, w_up, w_down):
        layers, rows, seq, _, head_dim = k_cache.shape
        d_model = hidden.shape[1]
        width = d_model // n_dev
        qkv_cols = w_qkv.shape[3]
        group = qkv_cols // head_dim - 2
        ff = w_gate.shape[2]
        half = rows // 2
        wide = CORES * width
        heads = group * head_dim
        inv_freq = (ROPE_BASE ** (-np.arange(0, head_dim, 2, dtype=np.float32) / head_dim)).astype(np.float32)
        freq = jnp.asarray(np.concatenate([inv_freq, inv_freq])[None, :])
        cfg = (layers, rows, width, head_dim, group, chips, seq)
        vmem = pl.BlockSpec(memory_space=pltpu.VMEM)
        hbm = pl.BlockSpec(memory_space=pl.ANY)
        flops = 2 * layers * rows * d_model * (qkv_cols + heads + 3 * ff)
        return emit(pl.pallas_call(
            functools.partial(kernel, cfg),
            out_shape=jax.ShapeDtypeStruct((rows, d_model), BF16),
            in_specs=[hbm] + [vmem] * 4 + [hbm] * 7,
            out_specs=hbm,
            scratch_shapes=[
                pltpu.VMEM((chips, CORES, rows, width), BF16),
                pltpu.VMEM((rows, wide), BF16),
                pltpu.VMEM((rows, 128), F32),
                pltpu.VMEM((rows * group, seq), F32),
                pltpu.VMEM((chips, CORES, rows, width), BF16),
                pltpu.VMEM((2, CORES, half, width), BF16),
                pltpu.VMEM((2, half, width), BF16),
                pltpu.VMEM((2, CORES, half, width), BF16),
                pltpu.VMEM((rows, width), BF16),
                pltpu.VMEM((2, half, width), F32),
                pltpu.VMEM((2, half, width), F32),
                pltpu.VMEM((n_dev, 8, rows), F32),
                pltpu.VMEM((rows, 128), F32),
                pltpu.VMEM((rows, head_dim), F32),
                pltpu.VMEM((rows, head_dim), F32),
                pltpu.VMEM((rows * group, head_dim), F32),
                pltpu.VMEM((rows * group, head_dim), F32),
                pltpu.VMEM((rows * group, head_dim), F32),
                pltpu.VMEM((rows * group, seq), F32),
                pltpu.VMEM((rows, heads), BF16),
                pltpu.VMEM((rows, ff), BF16),
                pltpu.VMEM((rows, ff), F32),
                pltpu.VMEM((rows, ff), F32),
                pltpu.VMEM((rows, seq, head_dim), BF16),
                pltpu.VMEM((GU_SLOTS, wide, ff), BF16),
                pltpu.VMEM((chips, ff, wide), BF16),
                pltpu.SemaphoreType.DMA((3,)),
                pltpu.SemaphoreType.DMA((2, CORES, SPLIT)),
                pltpu.SemaphoreType.DMA((2, CORES, SPLIT)),
                pltpu.SemaphoreType.DMA((2, SPLIT)),
                pltpu.SemaphoreType.DMA((chips, CORES, 2, SPLIT)),
                pltpu.SemaphoreType.DMA((chips,)),
                pltpu.SemaphoreType.DMA((n_dev,)),
                pltpu.SemaphoreType.DMA((3 + 10 * SPLIT,)),
                pltpu.SemaphoreType.DMA((n_dev + 3 + 6 * SPLIT,)),
                pltpu.SemaphoreType.DMA((13,)),
                pltpu.SemaphoreType.DMA((16,)),
                pltpu.SemaphoreType.DMA((V_PARTS,)),
                pltpu.SemaphoreType.DMA((GU_SLOTS,)),
                pltpu.SemaphoreType.DMA((chips, CORES)),
            ],
            compiler_params=pltpu.CompilerParams(
                collective_id=0, has_side_effects=True, vmem_limit_bytes=67043328),
            cost_estimate=pl.CostEstimate(flops=flops, bytes_accessed=flops // rows, transcendentals=0),
        )(hidden, lengths.reshape(1, rows), freq, attn_norm, mlp_norm,
          w_qkv.reshape(layers, d_model, qkv_cols), w_out, w_gate, w_up, w_down,
          k_cache.reshape(layers, rows * seq, head_dim), v_cache.reshape(layers, rows, seq, head_dim)))

    cache_spec = P(None, 'dp', None, 'tp', None)
    in_specs = (P('dp', None), P('dp'), cache_spec, cache_spec, P(), P(None, None, 'tp', None),
                P(None, 'tp', None), P(), P(None, None, 'tp'), P(None, None, 'tp'), P(None, 'tp', None))
    return jax.shard_map(local_step, mesh=mesh, in_specs=in_specs, out_specs=P('dp', None), check_vma=False)
```
